32 devices in a mesh: dp: 2 (over x), tm: 4 (over z), mp: 4 (over y, core).
Axes of the slice: x: 2, y: 2, z: 4, core: 2. Of those that a mesh axis runs over, the one named last changes fastest.
Arguments:
- features: bfloat16 [32, 576, 1024], P(('dp', 'tm'), 'mp'), parts along dimension 0, may hold values from -6 to 6
- queries: bfloat16 [2048, 1024], P(('dp', 'tm')), parts along dimension 0, may hold values from -6 to 6
- anchor_frame: int32 [2048], P(('dp', 'tm')), parts along dimension 0, may hold values from 0 to 15, as said below
- anchor_patch: int32 [2048], P(('dp', 'tm')), parts along dimension 0, may hold values from 0 to 575
- time_offset: float32 [2048, 8, 4], P(('dp', 'tm')), parts along dimension 0, may hold values from -1.99 to 1.99
- space_offset: float32 [2, 2048, 8, 4], P(None, ('dp', 'tm')), parts along dimension 1, may hold values from -3 to 3
- value_weight: bfloat16 [1024, 1024], replicated, may hold values from -0.1875 to 0.1875
- point_weight: bfloat16 [1024, 32], replicated, may hold values from -0.1875 to 0.1875
- point_bias: float32 [32], replicated, may hold values from -6 to 260
- output_weight: bfloat16 [1024, 1024], P('mp'), may hold values from -0.1875 to 0.1875
- project_weight: bfloat16 [1024, 3584], P(None, 'mp'), may hold values from -2 to 2
- norm_gain: float32 [3584], P('mp'), may hold values from 0.1 to 1.9
- query_weight: bfloat16 [3584, 3072], P(None, 'mp'), may hold values from -0.09375 to 0.09375
- query_bias: float32 [3072], P('mp'), may hold values from -6 to 40
- cache_weight: bfloat16 [3584, 1024], P(None, 'mp'), may hold values from -0.09375 to 0.09375
- cache_bias: float32 [1024], P('mp'), may hold values from -6 to 40
Outputs:
- attention: bfloat16 [2048, 3072], P(('dp', 'tm'), 'mp'), parts along dimension 0
- key_value: bfloat16 [2048, 1024], P(('dp', 'tm'), 'mp'), parts along dimension 0
The draws below stay inside these ranges and needn't reach their ends.
There are 2 independent parts, one for each index of `dp`. The reference program is written for one: setup_inputs(seed, part) draws one part's arguments, and reference() takes and returns one part's arrays. A program takes and returns all parts, laid end to end along the dimension named above; an argument that names none is the same for every part. Nothing has to cross between parts.
Inputs may be any that keep to these rules, and one draw needn't show every extreme that they name: `anchor_frame`: the anchor frame of query q lies among the 4 frames that begin at (q // 256) * 4.
All inputs are finite; a program needn't handle non-finite values.
Results may differ from the reference program's by a relative error of at most 0.04.
Values may be sent and summed in bfloat16 or wider, within the bound.
A program may use at most 64 MiB of HBM per device.

```python
import math
import jax
import jax.numpy as jnp
from jax import lax

C = 1024
AH = 8
AHD = 128
POINTS = 4
GRID = 24
PATCH = 576
D = 3584
HEADS = 24
KVH = 4
HD = 128
GROUP = 7
FR_DEV = 4
Q_DEV = 256
FRAMES = 16
QUERIES = 1024


def draw_queries(key, part):
    normal_part = jnp.clip(jax.random.normal(key, (QUERIES, C), jnp.float32), -6.0, 6.0)
    normal_part = normal_part * 0.3
    return normal_part.astype(jnp.bfloat16)


def draw_anchor_frame(key, part):
    position = jnp.arange(QUERIES, dtype=jnp.int32)
    within = jax.random.randint(key, (QUERIES,), 0, FR_DEV, dtype=jnp.int32)
    return position // Q_DEV * FR_DEV + within


def draw_point_bias(key, part):
    normal_part = jnp.clip(jax.random.normal(key, (AH, POINTS), jnp.float32), -6.0, 6.0)
    return normal_part.reshape(AH * POINTS)


def draw_project_weight(key, part):
    normal_part = jnp.clip(jax.random.normal(key, (C, D), jnp.float32), -6.0, 6.0) / math.sqrt(C)
    column_scale = 1.0 + 4.0 * jnp.arange(D, dtype=jnp.float32) / D
    return jnp.clip(normal_part * column_scale[None, :], -2.0, 2.0).astype(jnp.bfloat16)


def draw_query_bias(key, part):
    normal_part = jnp.clip(jax.random.normal(jax.random.fold_in(key, 1), (HEADS, HD), jnp.float32), -6.0, 6.0)
    return normal_part.reshape(HEADS * HD)


def draw_cache_bias(key, part):
    normal_part = jnp.clip(jax.random.normal(jax.random.fold_in(key, 2), (2 * KVH, HD), jnp.float32), -6.0, 6.0)
    return normal_part.reshape(2 * KVH * HD)


def touch_ends(entries, rng, least, largest):
    place = [jax.random.randint(jax.random.fold_in(rng, axis), (), 0, length) for axis, length in enumerate(entries.shape)]
    longest = entries.shape.index(max(entries.shape))
    beside = place[:longest] + [(place[longest] + 1) % entries.shape[longest]] + place[longest + 1:]
    return entries.at[tuple(place)].set(least).at[tuple(beside)].set(largest)


def block_levels(own_key, extent, shards, low, top_value):
    loudness, own = 1.0, jax.random.fold_in(own_key, 6)
    for dim, blocks in shards:
        steps = jnp.exp(jax.random.uniform(jax.random.fold_in(own, dim), (blocks,), jnp.float32, low / len(shards), top_value / len(shards)))
        loudness = loudness * jnp.repeat(steps, extent[dim] // blocks).reshape([-1 if axis == dim else 1 for axis in range(len(extent))])
    return loudness


def gaussian(key, shape, width, most, split=(), kind=jnp.bfloat16):
    values = jax.random.normal(key, shape, jnp.float32) * width
    if len(split) > 0:
        values = block_levels(key, shape, split, -0.22, 0.18) * values
    return jnp.clip(values, min=-most, max=most).astype(kind)


def setup_inputs(seed: int = 0, part: int = 0) -> dict:
    seeds = jax.random.split(jax.random.key(seed), 17)
    part_splits = jax.random.split(jax.random.fold_in(seeds[16], part), 17)
    return {
        "features": gaussian(part_splits[0], (FRAMES, PATCH, C), 1.0, 6.0, ((0, 4), (1, 4))),
        "queries": draw_queries(jax.random.fold_in(jax.random.fold_in(seeds[16], part), 71), part),
        "anchor_frame": draw_anchor_frame(jax.random.fold_in(jax.random.fold_in(seeds[16], part), 71), part),
        "anchor_patch": touch_ends(jax.random.randint(part_splits[3], (QUERIES,), 0, PATCH), jax.random.fold_in(part_splits[3], 1), 0, PATCH - 1).astype(jnp.int32),
        "time_offset": jnp.clip(jax.random.uniform(part_splits[4], (QUERIES, AH, POINTS), jnp.float32, -1.99, 1.99) * block_levels(part_splits[4], (QUERIES, AH, POINTS), ((0, 4),), -0.4, 0.0), -1.99, 1.99),
        "space_offset": jnp.clip(jax.random.uniform(part_splits[5], (2, QUERIES, AH, POINTS), jnp.float32, -3.0, 3.0) * block_levels(part_splits[5], (2, QUERIES, AH, POINTS), ((1, 4),), -0.4, 0.0), -3.0, 3.0),
        "value_weight": gaussian(seeds[6], (C, C), C ** -0.5, 0.1875),
        "point_weight": gaussian(seeds[7], (C, AH * POINTS), C ** -0.5, 0.1875),
        "point_bias": draw_point_bias(jax.random.fold_in(seeds[16], 71), part),
        "output_weight": gaussian(seeds[9], (C, C), C ** -0.5, 0.1875, ((0, 4),)),
        "project_weight": draw_project_weight(jax.random.fold_in(seeds[16], 71), part),
        "norm_gain": jnp.clip(1.0 + 0.18 * jax.random.normal(seeds[11], (D,), jnp.float32), 0.1, 1.9),
        "query_weight": gaussian(seeds[12], (D, HEADS * HD), D ** -0.5, 0.09375, ((1, 4),)),
        "query_bias": draw_query_bias(jax.random.fold_in(seeds[16], 71), part),
        "cache_weight": gaussian(seeds[14], (D, 2 * KVH * HD), D ** -0.5, 0.09375, ((1, 4),)),
        "cache_bias": draw_cache_bias(jax.random.fold_in(seeds[16], 71), part),
    }


rope_base = 1000000.0
epsilon = 1e-06
masked = -1e+30

def rotate(vectors, positions):
    half_width = vectors.shape[-1] // 2
    frequency = rope_base ** (-2.0 * jnp.arange(half_width, dtype=jnp.float32) / vectors.shape[-1])
    angles = positions.astype(jnp.float32)[:, None] * frequency[None, :]
    cosine = jnp.cos(angles)[:, None, :]
    sine_part = jnp.sin(angles)[:, None, :]
    first_half = vectors[..., :half_width]
    second_half = vectors[..., half_width:]
    return jnp.concatenate([first_half * cosine - second_half * sine_part, second_half * cosine + first_half * sine_part], axis=-1)

def trilinear_corners(frame_pos, row_pos, column_pos, weight, frame_total, side):
    floor_frame = jnp.floor(frame_pos)
    floor_row = jnp.floor(row_pos)
    floor_column = jnp.floor(column_pos)
    frame_part = frame_pos - floor_frame
    row_part = row_pos - floor_row
    column_part = column_pos - floor_column
    frame_start = floor_frame.astype(jnp.int32)
    row_start = floor_row.astype(jnp.int32)
    column_start = floor_column.astype(jnp.int32)
    listing = []
    for frame_step in (0, 1):
        for row_step in (0, 1):
            for column_step in (0, 1):
                frame_cell = frame_start + frame_step
                row_cell = row_start + row_step
                column_cell = column_start + column_step
                portion = weight * (frame_part if frame_step else 1.0 - frame_part)
                portion = portion * (row_part if row_step else 1.0 - row_part)
                portion = portion * (column_part if column_step else 1.0 - column_part)
                inside = (frame_cell >= 0) & (frame_cell < frame_total) & (row_cell >= 0) & (row_cell < side)
                inside = inside & (column_cell >= 0) & (column_cell < side)
                portion = jnp.where(inside, portion, 0.0)
                patch_id = jnp.clip(row_cell, 0, side - 1) * side + jnp.clip(column_cell, 0, side - 1)
                listing.append((frame_cell, patch_id.astype(jnp.int32), portion))
    return listing

def reference(features, queries, anchor_frame, anchor_patch, time_offset, space_offset, value_weight, point_weight, point_bias, output_weight, project_weight, norm_gain, query_weight, query_bias, cache_weight, cache_bias):
    patch_values = jnp.dot(features.reshape(FRAMES * PATCH, C), value_weight, preferred_element_type=jnp.float32).astype(jnp.bfloat16)
    by_head = patch_values.reshape(FRAMES * PATCH, AH, AHD).transpose(1, 0, 2)
    logits = jnp.dot(queries, point_weight, preferred_element_type=jnp.float32) + point_bias
    point_share = jax.nn.softmax(logits.reshape(QUERIES, AH, POINTS), axis=-1)
    frame_pos = anchor_frame.astype(jnp.float32)[:, None, None] + time_offset
    row_pos = (anchor_patch // GRID).astype(jnp.float32)[:, None, None] + space_offset[0]
    column_pos = (anchor_patch % GRID).astype(jnp.float32)[:, None, None] + space_offset[1]

    def sample_head(inputs):
        lookup, frame_head, row_head, column_head, share_head = inputs
        running = jnp.zeros((QUERIES, AHD), jnp.float32)
        for frame_cell, patch_id, portion in trilinear_corners(frame_head, row_head, column_head, share_head, FRAMES, GRID):
            picked = lookup[jnp.clip(frame_cell, 0, FRAMES - 1) * PATCH + patch_id]
            running = running + lax.optimization_barrier(jnp.sum(portion[..., None] * picked.astype(jnp.float32), axis=1))
        return running
    sampled = lax.map(sample_head, (by_head, frame_pos.transpose(1, 0, 2), row_pos.transpose(1, 0, 2), column_pos.transpose(1, 0, 2), point_share.transpose(1, 0, 2)))
    sampled = sampled.transpose(1, 0, 2).reshape(QUERIES, C).astype(jnp.bfloat16)
    abstract = (queries.astype(jnp.float32) + jnp.dot(sampled, output_weight, preferred_element_type=jnp.float32)).astype(jnp.bfloat16)
    visual = jnp.dot(abstract, project_weight, preferred_element_type=jnp.float32)
    normed = (visual * lax.rsqrt(lax.optimization_barrier(jnp.mean(visual * visual, axis=1, keepdims=True)) + epsilon) * norm_gain).astype(jnp.bfloat16)
    positions = jnp.arange(QUERIES, dtype=jnp.int32)
    query_state = (jnp.dot(normed, query_weight, preferred_element_type=jnp.float32) + query_bias).reshape(QUERIES, HEADS, HD)
    query_state = rotate(query_state, positions).astype(jnp.bfloat16)
    cache_state = (jnp.dot(normed, cache_weight, preferred_element_type=jnp.float32) + cache_bias).reshape(QUERIES, 2 * KVH, HD)
    cache_state = jnp.concatenate([rotate(cache_state[:, :KVH], positions), cache_state[:, KVH:]], axis=1)
    key_value = cache_state.reshape(QUERIES, 2 * KVH * HD).astype(jnp.bfloat16)
    key_heads = key_value.reshape(QUERIES, 2 * KVH, HD).transpose(1, 0, 2)
    query_heads = query_state.transpose(1, 0, 2)
    allowed = positions[None, :] <= positions[:, None]

    def attend_head(head_id):
        group_id = head_id // GROUP
        scores = jnp.dot(query_heads[head_id], key_heads[group_id].T, preferred_element_type=jnp.float32) * HD ** (-0.5)
        scores = jnp.where(allowed, scores, masked)
        row_peak = lax.optimization_barrier(jnp.max(scores, axis=1, keepdims=True))
        weights = jnp.where(allowed, jnp.exp(scores - row_peak), 0.0)
        weighted = jnp.dot(weights.astype(jnp.bfloat16), key_heads[KVH + group_id], preferred_element_type=jnp.float32)
        return weighted / lax.optimization_barrier(jnp.sum(weights, axis=1, keepdims=True))
    attention = lax.map(attend_head, jnp.arange(HEADS, dtype=jnp.int32))
    attention = attention.transpose(1, 0, 2).reshape(QUERIES, HEADS * HD).astype(jnp.bfloat16)
    return (attention, key_value)
```

```python
import functools

import jax
import jax.numpy as jnp
import numpy as np
from jax import lax
from jax.experimental import pallas as pl
from jax.experimental.pallas import tpu as pltpu
from jax.sharding import PartitionSpec as P

AH = 8
POINTS = 4
GRID = 24
KVH = 4
HD = 128
GROUP = 7

rope_base = 1000000.0
epsilon = 1e-06
masked = -1e30
chunk_rows = 128
MESH = pl.DeviceIdType.MESH
BF = jnp.bfloat16
F32 = jnp.float32


def remote(src, dst, send, recv, device):
    return pltpu.make_async_remote_copy(
        src_ref=src, dst_ref=dst, send_sem=send, recv_sem=recv, device_id=device, device_id_type=MESH
    )


class Gather:
    def __init__(self, slot_ref, own, sems, groups, me):
        self.chips = groups // 2
        self.chip, self.core = me // 2, me % 2
        self.me, self.partner = me, me + 1 - 2 * (me % 2)
        cs, cr, ps, pr = sems
        self.cross = [None] + [
            remote(
                own,
                slot_ref(me),
                cs(d),
                cr(d),
                {"mp": (self.chip + d) % self.chips * 2 + self.core},
            )
            for d in range(1, self.chips)
        ]
        self.near = [remote(own, slot_ref(me), ps(0), pr(0), {"mp": self.partner})]
        for d in range(1, self.chips):
            slot = slot_ref(self.slot(d, self.core))
            self.near.append(remote(slot, slot, ps(d), pr(d), {"mp": self.partner}))

    def slot(self, d, core):
        return (self.chip + self.chips - d) % self.chips * 2 + core

    def start(self):
        for copy in self.cross[1:]:
            copy.start()
        self.near[0].start()

    def arrivals(self):
        self.near[0].wait_recv()
        yield self.partner
        for d in range(1, self.chips):
            self.cross[d].wait_recv()
            self.near[d].start()
            yield self.slot(d, self.core)
            self.near[d].wait_recv()
            yield self.slot(d, 1 - self.core)

    def drain(self):
        for copy in self.cross[1:] + self.near:
            copy.wait_send()


def shared_heads(groups, q_heads, ch):
    table = []
    for source in range(groups):
        for target in range(groups):
            wanted = {(target * q_heads + i) // GROUP for i in range(q_heads)}
            need = [h for h in range(ch) if (source * ch + h) % KVH in wanted]
            if target != source and need:
                table.append((source, target, need[0], need[-1] - need[0] + 1))
    return table


def flat(ref):
    return jnp.concatenate([ref[i : i + 1, :] for i in range(ref.shape[0])], axis=1)


def kernel(
    groups,
    spans,
    frames,
    chunks,
    features,
    queries_hbm,
    row_turn_hbm,
    anchor_frame,
    anchor_patch,
    time_offset,
    space_offset,
    point_weight,
    point_bias,
    span_turn,
    gain,
    query_bias,
    cache_bias,
    value_hbm,
    output_hbm,
    project_hbm,
    query_hbm,
    cache_hbm,
    attention,
    key_value,
    own_features,
    queries,
    row_turn,
    vw,
    wo,
    wp,
    wq,
    wc,
    halo,
    own_values,
    halo_values,
    logits,
    coords,
    cosine,
    sine,
    corner,
    partial,
    rs_send,
    rs_recv,
    ex,
    ab,
    vx,
    ssq,
    scale,
    q_acc,
    kv_acc,
    qs,
    kv,
    peak,
    denom,
    numer,
    load_sem,
    halo_ss,
    halo_rs,
    rs_ss,
    rs_rs,
    ex_ss,
    ex_rs,
    ab_ss,
    ab_rs,
    sq_ss,
    sq_rs,
    z_ss,
    z_rs,
    d_ss,
    d_rs,
    ag_sem,
):
    me = lax.axis_index("mp")
    t = lax.axis_index("tm")
    cells, width = features.shape
    rows = queries.shape[0]
    per_frame = cells // frames
    lines = per_frame // GRID
    model = wp.shape[1]
    q_width = wq.shape[1]
    q_heads = qs.shape[0]
    ch = kv.shape[3] // HD
    chips = groups // 2
    chip, core = me // 2, me % 2
    partner = me + 1 - 2 * core
    size = rows // chunks
    part = size // 2

    loads = [
        pltpu.make_async_copy(src, dst, load_sem.at[i])
        for i, (src, dst) in enumerate(
            [
                (queries_hbm, queries),
                (features, own_features),
                (value_hbm, vw),
                (output_hbm, wo.at[me]),
                (row_turn_hbm, row_turn),
                (project_hbm, wp),
                (cache_hbm, wc),
                (query_hbm, wq),
            ]
        )
    ]
    for load in loads:
        load.start()

    barrier = pltpu.get_barrier_semaphore()
    for d in range(1, groups):
        pl.semaphore_signal(barrier, inc=1, device_id={"mp": (me + d) % groups}, device_id_type=MESH)

    @pl.when(t < spans - 1)
    def _():
        pl.semaphore_signal(barrier, inc=1, device_id={"tm": (t + 1) % spans}, device_id_type=MESH)

    @pl.when(t > 0)
    def _():
        pl.semaphore_signal(barrier, inc=1, device_id={"tm": (t + spans - 1) % spans}, device_id_type=MESH)

    neighbours = jnp.where(t > 0, 1, 0) + jnp.where(t < spans - 1, 1, 0)
    pl.semaphore_wait(barrier, groups - 1 + neighbours)

    up, down = [], []
    for i in range(2):
        up.append(
            remote(
                features.at[pl.ds((frames - 1 - i) * per_frame, per_frame)],
                halo.at[pl.ds(2 * i * per_frame, per_frame)],
                halo_ss.at[0, i],
                halo_rs.at[0, i],
                {"tm": (t + 1) % spans},
            )
        )
        down.append(
            remote(
                features.at[pl.ds(i * per_frame, per_frame)],
                halo.at[pl.ds((2 * i + 1) * per_frame, per_frame)],
                halo_ss.at[1, i],
                halo_rs.at[1, i],
                {"tm": (t + spans - 1) % spans},
            )
        )

    @pl.when(t < spans - 1)
    def _():
        for copy in up:
            copy.start()

    @pl.when(t > 0)
    def _():
        for copy in down:
            copy.start()

    def gather_sems(index):
        return [functools.partial(lambda k, d: ag_sem.at[index, k, d], k) for k in range(4)]

    wo_gather = Gather(lambda s: wo.at[s], output_hbm, gather_sems(0), groups, me)
    wo_gather.start()

    @pl.when(t == 0)
    def _():
        for i in range(2):
            halo[pl.ds(2 * i * per_frame, per_frame), :] = jnp.zeros((per_frame, width), BF)

    @pl.when(t == spans - 1)
    def _():
        for i in range(2):
            halo[pl.ds((2 * i + 1) * per_frame, per_frame), :] = jnp.zeros((per_frame, width), BF)

    loads[0].wait()
    logits[...] = jnp.zeros((rows, HD), F32)
    logits[:, 0 : AH * POINTS] = (
        lax.dot_general(
            queries[...], point_weight[...], (((1,), (1,)), ((), ())), preferred_element_type=F32
        )
        + point_bias[...]
    )
    by_point = logits[...].T
    frame_at = anchor_frame[...].astype(F32)
    patch = anchor_patch[...].astype(F32)
    row_at = jnp.floor((patch + 0.5) * (1.0 / GRID))
    column_at = patch - row_at * GRID
    for h in range(AH):
        own = by_point[h * POINTS : (h + 1) * POINTS]
        own = jnp.exp(own - jnp.max(own, axis=0, keepdims=True))
        coords[h, 0:4, :] = time_offset[h] + frame_at
        coords[h, 4:8, :] = space_offset[0, h] + row_at
        coords[h, 8:12, :] = space_offset[1, h] + column_at
        coords[h, 12:16, :] = own / jnp.sum(own, axis=0, keepdims=True)

    loads[1].wait()
    loads[2].wait()

    def project_values(source, target):
        for c in range(width // 256):
            cols = slice(c * 256, (c + 1) * 256)
            target[:, cols] = jnp.dot(source[...], vw[:, cols], preferred_element_type=F32).astype(BF)

    line_index = lax.broadcasted_iota(jnp.int32, (GRID, rows), 0).astype(F32)
    first_line = (me * lines).astype(F32)
    first_frame = (t * frames).astype(F32)

    def hat(position, cell):
        return jnp.maximum(1.0 - jnp.abs(position - cell), 0.0)

    def sample(values, offsets, head):
        info = coords[head]
        columns = [hat(info[8 + k : 9 + k], line_index) for k in range(POINTS)]
        for f, offset in enumerate(offsets):
            timed = info[12:16] * hat(info[0:4], first_frame + offset)
            for line in range(lines):
                share = timed * hat(info[4:8], first_line + line)
                total = share[0:1] * columns[0]
                for k in range(1, POINTS):
                    total = total + share[k : k + 1] * columns[k]
                corner[pl.ds((f * lines + line) * GRID, GRID), :] = total
        cols = pl.ds(pl.multiple_of(head * HD, HD), HD)
        return lax.dot_general(
            corner[pl.ds(0, values.shape[0]), :].astype(BF),
            values[:, cols],
            (((0,), (0,)), ((), ())),
            preferred_element_type=F32,
        )

    project_values(own_features, own_values)


    @pl.loop(0, AH)
    def _(head):
        cols = pl.ds(pl.multiple_of(head * HD, HD), HD)
        partial[:, cols] = sample(own_values, range(frames), head)

    loads[4].wait()
    span_cos, span_sin = span_turn[0, pl.ds(t, 1), :], span_turn[1, pl.ds(t, 1), :]
    cosine[...] = span_cos * row_turn[0] - span_sin * row_turn[1]
    sine[...] = span_sin * row_turn[0] + span_cos * row_turn[1]

    for i in range(2):

        @pl.when(t > 0)
        def _(i=i):
            up[i].wait_recv()

        @pl.when(t < spans - 1)
        def _(i=i):
            down[i].wait_recv()

        both = pl.ds(2 * i * per_frame, 2 * per_frame)
        project_values(halo.at[both], halo_values)

        @pl.loop(0, AH)
        def _(head, i=i):
            cols = pl.ds(pl.multiple_of(head * HD, HD), HD)
            partial[:, cols] = partial[:, cols] + sample(halo_values, (-1 - i, frames + i), head)

        if i == 0:
            loads[3].wait()
            for _ in wo_gather.arrivals():
                pass


    def rows_of(k, which):
        return pl.ds(pl.multiple_of(k * size + which * part, part), part)

    rs = []
    for k in range(chunks):
        rs_send[k] = partial[rows_of(k, 1 - core), :].astype(BF)
        rs.append(remote(rs_send.at[k], rs_recv.at[k], rs_ss.at[k], rs_rs.at[k], {"mp": partner}))
        rs[k].start()
    exchange = []
    for k in range(chunks):
        rs[k].wait_recv()
        ex[chip, k] = (partial[rows_of(k, core), :] + rs_recv[k].astype(F32)).astype(BF)
        copies = []
        for d in range(1, chips):
            mine = ex.at[chip, k]
            copies.append(
                remote(mine, mine, ex_ss.at[k, d], ex_rs.at[k, d], {"mp": (chip + d) % chips * 2 + core})
            )
            copies[-1].start()
        exchange.append(copies)
    loads[5].wait()

    def chunk_slice(k):
        return slice(k * size, (k + 1) * size)

    vx_gathers, ab_copies, sq = [], [], []
    for k in range(chunks):
        for copy in exchange[k]:
            copy.wait_recv()
        total = ex[0, k].astype(F32)
        for c in range(1, chips):
            total = total + ex[c, k].astype(F32)
        mixed = jnp.dot(total.astype(BF), wo[...].reshape(width, width), preferred_element_type=F32)
        ab[k, core] = (queries[rows_of(k, core), :].astype(F32) + mixed).astype(BF)
        mine = ab.at[k, core]
        ab_copies.append(remote(mine, mine, ab_ss.at[k], ab_rs.at[k], {"mp": partner}))
        ab_copies[k].start()
        ab_copies[k].wait_recv()
        visual = jnp.dot(ab[k].reshape(size, width), wp[...], preferred_element_type=F32)
        vx[me, chunk_slice(k), :] = (visual * flat(gain)).astype(BF)
        squares = jnp.broadcast_to(jnp.sum(visual * visual, axis=1, keepdims=True), (size, HD)).T
        ssq[k, 0] = squares[0:8]
        for d in range(1, groups):
            copy = remote(
                ssq.at[k, 0], ssq.at[k, d], sq_ss.at[k, d], sq_rs.at[k, d], {"mp": (me + d) % groups}
            )
            copy.start()
            sq.append(copy)
        gather = Gather(
            lambda s, k=k: vx.at[s, pl.ds(k * size, size)],
            vx.at[me, pl.ds(k * size, size)],
            gather_sems(1 + k),
            groups,
            me,
        )
        gather.start()
        vx_gathers.append(gather)

    tile = 256 if q_width % 256 == 0 else 128

    def slot_rows(slot):
        return pl.ds(pl.multiple_of(slot * model, 64), model)

    def add_cache(slot, span, first):
        term = jnp.dot(vx[slot, span, :], wc[slot_rows(slot), :], preferred_element_type=F32)
        kv_acc[span, :] = term if first else kv_acc[span, :] + term

    def add_query(slot, span, first):
        for c in range(q_width // tile):
            cols = slice(c * tile, (c + 1) * tile)
            term = jnp.dot(vx[slot, span, :], wq[slot_rows(slot), cols], preferred_element_type=F32)
            q_acc[span, cols] = term if first else q_acc[span, cols] + term

    def turn(x, cos, sin):
        return x * cos + pltpu.roll(x, HD // 2, 1) * sin

    def finish_cache(k):
        span = chunk_slice(k)
        square_sum = ssq[k, 0]
        for d in range(1, groups):
            sq[k * (groups - 1) + d - 1].wait_recv()
            square_sum = square_sum + ssq[k, d]
        scale_row = lax.rsqrt(square_sum * (1.0 / (model * groups)) + epsilon)
        scale[span, :] = jnp.broadcast_to(scale_row[0:1], (HD, size)).T
        bias = flat(cache_bias)
        for i in range(ch):
            is_key = me * ch + i < KVH
            cols = slice(i * HD, (i + 1) * HD)
            state = kv_acc[span, cols] * scale[span, :] + bias[:, cols]
            cos = jnp.where(is_key, cosine[span, :], 1.0)
            sin = jnp.where(is_key, sine[span, :], 0.0)
            state = turn(state, cos, sin).astype(BF)
            kv[t, me, span, cols] = state
            key_value[span, cols] = state

    def finish_query(k):
        span = chunk_slice(k)
        bias = flat(query_bias)
        for i in range(q_heads):
            cols = slice(i * HD, (i + 1) * HD)
            state = q_acc[span, cols] * scale[span, :] + bias[:, cols]
            qs[i, span, :] = turn(state, cosine[span, :], sine[span, :]).astype(BF)

    table = shared_heads(groups, q_heads, ch)

    def share_copy(d, k, entry):
        source, target, first, count = entry
        block = kv.at[
            lax.rem(t + spans - d, spans), source, pl.ds(k * size, size), pl.ds(first * HD, count * HD)
        ]
        return remote(block, block, d_ss.at[d, k, target], d_rs.at[d, k, source], {"mp": target})

    def share(d, k):
        for entry in table:

            @pl.when(me == entry[0])
            def _(entry=entry):
                share_copy(d, k, entry).start()

    def share_wait(d, k):
        for entry in table:

            @pl.when(me == entry[1])
            def _(entry=entry):
                share_copy(d, k, entry).wait_recv()

    def share_drain(d, k):
        for entry in table:

            @pl.when(me == entry[0])
            def _(entry=entry):
                share_copy(d, k, entry).wait_send()

    def pass_copy(d, k):
        block = kv.at[lax.rem(t + spans - d, spans), me, pl.ds(k * size, size)]
        return remote(block, block, z_ss.at[d, k], z_rs.at[d + 1, k], {"tm": (t + 1) % spans})

    def arrive_copy(d, k):
        block = kv.at[lax.rem(t + spans - d, spans), me, pl.ds(k * size, size)]
        return remote(block, block, z_ss.at[d, k], z_rs.at[d, k], {"tm": (t + spans - 1) % spans})

    def hand_on(d, k):
        @pl.when(t < spans - 1)
        def _():
            pass_copy(d, k).start()

        share(d, k)

    def service(d, k):
        arrive_copy(d, k).wait_recv()
        hand_on(d, k)

    loads[6].wait()
    loads[7].wait()
    everything = slice(0, rows)
    add_cache(me, everything, True)
    add_query(me, everything, True)
    arrivals = [gather.arrivals() for gather in vx_gathers]
    for k in range(chunks):
        slot = next(arrivals[k])
    add_cache(slot, everything, False)
    add_query(slot, everything, False)
    for k in range(chunks):
        span = chunk_slice(k)
        slots = []
        for slot in arrivals[k]:
            add_cache(slot, span, False)
            slots.append(slot)
        finish_cache(k)
        hand_on(0, k)
        for slot in slots:
            add_query(slot, span, False)
        finish_query(k)
        if k == 0 and chunks > 1:

            @pl.when(t > 0)
            def _():
                service(1, 0)

    def service_all(d):
        for k in range(chunks):
            if k == 0 and chunks > 1:

                @pl.when(d > 1)
                def _():
                    service(d, 0)
            else:
                service(d, k)

    def attend(d, diagonal):
        j = lax.rem(t + spans - d, spans)

        @pl.loop(0, q_heads, unroll=3 if q_heads % 3 == 0 else 1)
        def _(i):
            g = (me * q_heads + i) // GROUP
            k_cols = pl.ds(pl.multiple_of(lax.rem(g, ch) * HD, HD), HD)
            keys = kv[j, g // ch, :, k_cols]
            values = kv[j, (KVH + g) // ch, :, pl.ds(pl.multiple_of(lax.rem(KVH + g, ch) * HD, HD), HD)]
            scores = lax.dot_general(
                qs[i], keys, (((1,), (1,)), ((), ())), preferred_element_type=F32
            ) * (HD ** -0.5 * 1.4426950408889634)
            if diagonal:
                q_pos = lax.broadcasted_iota(jnp.int32, (rows, rows), 0)
                k_pos = lax.broadcasted_iota(jnp.int32, (rows, rows), 1)
                scores = jnp.where(k_pos <= q_pos, scores, masked)
            top = jnp.max(scores, axis=1, keepdims=True)
            if diagonal:
                new_peak = jnp.broadcast_to(top, (rows, HD))
            else:
                new_peak = jnp.maximum(peak[i], top)
            weights = jnp.exp2(scores - new_peak[:, 0:1])
            added = jnp.sum(weights, axis=1, keepdims=True)
            product = jnp.dot(weights.astype(BF), values, preferred_element_type=F32)
            if diagonal:
                denom[i] = jnp.broadcast_to(added, (rows, HD))
                numer[i] = product
            else:
                rescale = jnp.exp2(peak[i] - new_peak)
                denom[i] = denom[i] * rescale + added
                numer[i] = numer[i] * rescale + product
            peak[i] = new_peak

    def share_wait_all(d):
        for k in range(chunks):
            share_wait(d, k)

    last = t == spans - 1

    @pl.when(t < spans - 1)
    def _():
        @pl.loop(1, t + 1)
        def _(d):
            service_all(d)

    @pl.when(last)
    def _():
        service_all(1)

    share_wait_all(0)
    attend(0, True)

    @pl.loop(1, t + 1)
    def _(d):
        @pl.when(last & (d < t))
        def _():
            service_all(d + 1)

        share_wait_all(d)
        attend(d, False)

    for i in range(q_heads):
        attention[:, i * HD : (i + 1) * HD] = (numer[i] / denom[i]).astype(BF)


    @pl.when(t < spans - 1)
    def _():
        for copy in up:
            copy.wait_send()

        @pl.loop(0, t + 1)
        def _(d):
            for k in range(chunks):
                pass_copy(d, k).wait_send()

    @pl.when(t > 0)
    def _():
        for copy in down:
            copy.wait_send()

    @pl.loop(0, t + 1)
    def _(d):
        for k in range(chunks):
            share_drain(d, k)

    wo_gather.drain()
    for gather in vx_gathers:
        gather.drain()
    for copy in rs + ab_copies + sq:
        copy.wait_send()
    for copies in exchange:
        for copy in copies:
            copy.wait_send()


def rows_first(x):
    return x.reshape(-1, HD) if x.shape[0] % HD == 0 else x[None]


def local(
    features,
    queries,
    anchor_frame,
    anchor_patch,
    time_offset,
    space_offset,
    value_weight,
    point_weight,
    point_bias,
    output_weight,
    project_weight,
    norm_gain,
    query_weight,
    query_bias,
    cache_weight,
    cache_bias,
):
    groups = lax.axis_size("mp")
    spans = lax.axis_size("tm")
    frames_here, patches_here, width = features.shape
    cells = frames_here * patches_here
    rows = queries.shape[0]
    chunks = max(1, rows // chunk_rows)
    size = rows // chunks
    part = size // 2
    frequency = rope_base ** (-2.0 * np.arange(HD // 2, dtype=np.float64) / HD)
    sign = np.concatenate([-np.ones(HD // 2), np.ones(HD // 2)])

    def turns(positions):
        angles = positions[:, None] * np.concatenate([frequency, frequency])[None, :]
        return jnp.asarray(np.stack([np.cos(angles), np.sin(angles) * sign]).astype(np.float32))

    row_turn = turns(np.arange(rows, dtype=np.float64))
    span_turn = turns(np.arange(spans, dtype=np.float64) * rows)
    model = project_weight.shape[1]
    q_width = query_weight.shape[1]
    c_width = cache_weight.shape[1]
    q_heads = q_width // HD
    chips = groups // 2
    vmem = pl.BlockSpec(memory_space=pltpu.VMEM)
    hbm = pl.BlockSpec(memory_space=pltpu.HBM)
    dma = pltpu.SemaphoreType.DMA
    V = pltpu.VMEM
    return tuple(
        pl.pallas_call(
            functools.partial(kernel, groups, spans, frames_here, chunks),
            out_shape=(
                jax.ShapeDtypeStruct((rows, q_width), BF),
                jax.ShapeDtypeStruct((rows, c_width), BF),
            ),
            in_specs=[hbm] * 3 + [vmem] * 10 + [hbm] * 5,
            out_specs=(vmem, vmem),
            scratch_shapes=[
                V((cells, width), BF),
                V((rows, width), BF),
                V((2, rows, HD), F32),
                V((width, width), BF),
                V((groups, width // groups, width), BF),
                V((width, model), BF),
                V(query_weight.shape, BF),
                V(cache_weight.shape, BF),
                V((4 * patches_here, width), BF),
                V((cells, width), BF),
                V((2 * patches_here, width), BF),
                V((rows, HD), F32),
                V((AH, 4 * POINTS, rows), F32),
                V((rows, HD), F32),
                V((rows, HD), F32),
                V((max(2, frames_here) * patches_here, rows), F32),
                V((rows, width), F32),
                V((chunks, part, width), BF),
                V((chunks, part, width), BF),
                V((chips, chunks, part, width), BF),
                V((chunks, 2, part, width), BF),
                V((groups, rows, model), BF),
                V((chunks, groups, 8, size), F32),
                V((rows, HD), F32),
                V((rows, q_width), F32),
                V((rows, c_width), F32),
                V((q_heads, rows, HD), BF),
                V((spans, groups, rows, c_width), BF),
                V((q_heads, rows, HD), F32),
                V((q_heads, rows, HD), F32),
                V((q_heads, rows, HD), F32),
                dma((8,)),
                dma((2, 2)),
                dma((2, 2)),
                dma((chunks,)),
                dma((chunks,)),
                dma((chunks, chips)),
                dma((chunks, chips)),
                dma((chunks,)),
                dma((chunks,)),
                dma((chunks, groups)),
                dma((chunks, groups)),
                dma((spans, chunks)),
                dma((spans, chunks)),
                dma((spans, chunks, groups)),
                dma((spans, chunks, groups)),
                dma((1 + chunks, 4, chips)),
            ],
            compiler_params=pltpu.CompilerParams(
                collective_id=0, has_side_effects=True, vmem_limit_bytes=48 * 1024 * 1024
            ),
        )(
            features.reshape(cells, width),
            queries,
            row_turn,
            anchor_frame[None],
            anchor_patch[None],
            time_offset.transpose(1, 2, 0),
            space_offset.transpose(0, 2, 3, 1),
            point_weight.T,
            point_bias[None],
            span_turn,
            rows_first(norm_gain),
            rows_first(query_bias),
            rows_first(cache_bias),
            value_weight,
            output_weight,
            project_weight,
            query_weight,
            cache_weight,
        )
    )


def solution(mesh):
    return jax.shard_map(
        local,
        mesh=mesh,
        in_specs=(
            P(("dp", "tm"), "mp", None),
            P(("dp", "tm"), None),
            P(("dp", "tm")),
            P(("dp", "tm")),
            P(("dp", "tm"), None, None),
            P(None, ("dp", "tm"), None, None),
            P(),
            P(),
            P(),
            P("mp", None),
            P(None, "mp"),
            P("mp"),
            P(None, "mp"),
            P("mp"),
            P(None, "mp"),
            P("mp"),
        ),
        out_specs=(P(("dp", "tm"), "mp"), P(("dp", "tm"), "mp")),
        check_vma=False,
    )
```

```python
import functools

import jax
import jax.numpy as jnp
import numpy as np
from jax import lax
from jax.experimental import pallas as pl
from jax.experimental.pallas import tpu as pltpu
from jax.sharding import PartitionSpec as P

AH = 8
POINTS = 4
GRID = 24
KVH = 4
HD = 128
GROUP = 7

rope_base = 1000000.0
epsilon = 1e-06
masked = -1e30
chunk_rows = 128
MESH = pl.DeviceIdType.MESH
BF = jnp.bfloat16
F32 = jnp.float32


def remote(src, dst, send, recv, device):
    return pltpu.make_async_remote_copy(
        src_ref=src, dst_ref=dst, send_sem=send, recv_sem=recv, device_id=device, device_id_type=MESH
    )


class Gather:
    def __init__(self, slot_ref, own, sems, groups, me):
        self.chips = groups // 2
        self.chip, self.core = me // 2, me % 2
        self.me, self.partner = me, me + 1 - 2 * (me % 2)
        cs, cr, ps, pr = sems
        self.cross = [None] + [
            remote(
                own,
                slot_ref(me),
                cs(d),
                cr(d),
                {"mp": (self.chip + d) % self.chips * 2 + self.core},
            )
            for d in range(1, self.chips)
        ]
        self.near = [remote(own, slot_ref(me), ps(0), pr(0), {"mp": self.partner})]
        for d in range(1, self.chips):
            slot = slot_ref(self.slot(d, self.core))
            self.near.append(remote(slot, slot, ps(d), pr(d), {"mp": self.partner}))

    def slot(self, d, core):
        return (self.chip + self.chips - d) % self.chips * 2 + core

    def start(self):
        for copy in self.cross[1:]:
            copy.start()
        self.near[0].start()

    def arrivals(self):
        self.near[0].wait_recv()
        yield self.partner
        for d in range(1, self.chips):
            self.cross[d].wait_recv()
            self.near[d].start()
            yield self.slot(d, self.core)
            self.near[d].wait_recv()
            yield self.slot(d, 1 - self.core)

    def drain(self):
        for copy in self.cross[1:] + self.near:
            copy.wait_send()


def shared_heads(groups, q_heads, ch):
    table = []
    for source in range(groups):
        for target in range(groups):
            wanted = {(target * q_heads + i) // GROUP for i in range(q_heads)}
            need = [h for h in range(ch) if (source * ch + h) % KVH in wanted]
            if target != source and need:
                table.append((source, target, need[0], need[-1] - need[0] + 1))
    return table


def flat(ref):
    return jnp.concatenate([ref[i : i + 1, :] for i in range(ref.shape[0])], axis=1)


def kernel(
    groups,
    spans,
    frames,
    chunks,
    features,
    queries_hbm,
    row_turn_hbm,
    anchor_frame,
    anchor_patch,
    time_offset,
    space_offset,
    point_weight,
    point_bias,
    span_turn,
    gain,
    query_bias,
    cache_bias,
    value_hbm,
    output_hbm,
    project_hbm,
    query_hbm,
    cache_hbm,
    attention,
    key_value,
    own_features,
    queries,
    row_turn,
    vw,
    wo,
    wp,
    wq,
    wc,
    halo,
    own_values,
    halo_values,
    logits,
    coords,
    cosine,
    sine,
    corner,
    partial,
    rs_send,
    rs_recv,
    ex,
    ab,
    vx,
    ssq,
    scale,
    q_acc,
    kv_acc,
    qs,
    kv,
    peak,
    denom,
    numer,
    load_sem,
    halo_ss,
    halo_rs,
    rs_ss,
    rs_rs,
    ex_ss,
    ex_rs,
    ab_ss,
    ab_rs,
    sq_ss,
    sq_rs,
    z_ss,
    z_rs,
    d_ss,
    d_rs,
    ag_sem,
):
    me = lax.axis_index("mp")
    t = lax.axis_index("tm")
    cells, width = features.shape
    rows = queries.shape[0]
    per_frame = cells // frames
    lines = per_frame // GRID
    model = wp.shape[1]
    q_width = wq.shape[1]
    q_heads = qs.shape[0]
    ch = kv.shape[3] // HD
    chips = groups // 2
    chip, core = me // 2, me % 2
    partner = me + 1 - 2 * core
    size = rows // chunks
    part = size // 2

    loads = [
        pltpu.make_async_copy(src, dst, load_sem.at[i])
        for i, (src, dst) in enumerate(
            [
                (queries_hbm, queries),
                (features, own_features),
                (value_hbm, vw),
                (output_hbm, wo.at[me]),
                (row_turn_hbm, row_turn),
                (project_hbm, wp),
                (cache_hbm, wc),
                (query_hbm, wq),
            ]
        )
    ]
    for load in loads:
        load.start()

    barrier = pltpu.get_barrier_semaphore()
    for d in range(1, groups):
        pl.semaphore_signal(barrier, inc=1, device_id={"mp": (me + d) % groups}, device_id_type=MESH)

    @pl.when(t < spans - 1)
    def _():
        pl.semaphore_signal(barrier, inc=1, device_id={"tm": (t + 1) % spans}, device_id_type=MESH)

    @pl.when(t > 0)
    def _():
        pl.semaphore_signal(barrier, inc=1, device_id={"tm": (t + spans - 1) % spans}, device_id_type=MESH)

    neighbours = jnp.where(t > 0, 1, 0) + jnp.where(t < spans - 1, 1, 0)
    pl.semaphore_wait(barrier, groups - 1 + neighbours)

    up, down = [], []
    for i in range(2):
        up.append(
            remote(
                features.at[pl.ds((frames - 1 - i) * per_frame, per_frame)],
                halo.at[pl.ds(2 * i * per_frame, per_frame)],
                halo_ss.at[0, i],
                halo_rs.at[0, i],
                {"tm": (t + 1) % spans},
            )
        )
        down.append(
            remote(
                features.at[pl.ds(i * per_frame, per_frame)],
                halo.at[pl.ds((2 * i + 1) * per_frame, per_frame)],
                halo_ss.at[1, i],
                halo_rs.at[1, i],
                {"tm": (t + spans - 1) % spans},
            )
        )

    @pl.when(t < spans - 1)
    def _():
        for copy in up:
            copy.start()

    @pl.when(t > 0)
    def _():
        for copy in down:
            copy.start()

    def gather_sems(index):
        return [functools.partial(lambda k, d: ag_sem.at[index, k, d], k) for k in range(4)]

    wo_gather = Gather(lambda s: wo.at[s], output_hbm, gather_sems(0), groups, me)
    wo_gather.start()

    @pl.when(t == 0)
    def _():
        for i in range(2):
            halo[pl.ds(2 * i * per_frame, per_frame), :] = jnp.zeros((per_frame, width), BF)

    @pl.when(t == spans - 1)
    def _():
        for i in range(2):
            halo[pl.ds((2 * i + 1) * per_frame, per_frame), :] = jnp.zeros((per_frame, width), BF)

    loads[0].wait()
    logits[...] = jnp.zeros((rows, HD), F32)
    logits[:, 0 : AH * POINTS] = (
        lax.dot_general(
            queries[...], point_weight[...], (((1,), (1,)), ((), ())), preferred_element_type=F32
        )
        + point_bias[...]
    )
    by_point = logits[...].T
    frame_at = anchor_frame[...].astype(F32)
    patch = anchor_patch[...].astype(F32)
    row_at = jnp.floor((patch + 0.5) * (1.0 / GRID))
    column_at = patch - row_at * GRID
    for h in range(AH):
        own = by_point[h * POINTS : (h + 1) * POINTS]
        own = jnp.exp(own - jnp.max(own, axis=0, keepdims=True))
        coords[h, 0:4, :] = time_offset[h] + frame_at
        coords[h, 4:8, :] = space_offset[0, h] + row_at
        coords[h, 8:12, :] = space_offset[1, h] + column_at
        coords[h, 12:16, :] = own / jnp.sum(own, axis=0, keepdims=True)

    loads[1].wait()
    loads[2].wait()

    def project_values(source, target):
        for c in range(width // 256):
            cols = slice(c * 256, (c + 1) * 256)
            target[:, cols] = jnp.dot(source[...], vw[:, cols], preferred_element_type=F32).astype(BF)

    line_index = lax.broadcasted_iota(jnp.int32, (GRID, rows), 0).astype(F32)
    first_line = (me * lines).astype(F32)
    first_frame = (t * frames).astype(F32)

    def hat(position, cell):
        return jnp.maximum(1.0 - jnp.abs(position - cell), 0.0)

    def sample(values, offsets, head):
        info = coords[head]
        columns = [hat(info[8 + k : 9 + k], line_index) for k in range(POINTS)]
        for f, offset in enumerate(offsets):
            timed = info[12:16] * hat(info[0:4], first_frame + offset)
            for line in range(lines):
                share = timed * hat(info[4:8], first_line + line)
                total = share[0:1] * columns[0]
                for k in range(1, POINTS):
                    total = total + share[k : k + 1] * columns[k]
                corner[pl.ds((f * lines + line) * GRID, GRID), :] = total
        cols = pl.ds(pl.multiple_of(head * HD, HD), HD)
        return lax.dot_general(
            corner[pl.ds(0, values.shape[0]), :].astype(BF),
            values[:, cols],
            (((0,), (0,)), ((), ())),
            preferred_element_type=F32,
        )

    project_values(own_features, own_values)


    @pl.loop(0, AH)
    def _(head):
        cols = pl.ds(pl.multiple_of(head * HD, HD), HD)
        partial[:, cols] = sample(own_values, range(frames), head)

    loads[4].wait()
    span_cos, span_sin = span_turn[0, pl.ds(t, 1), :], span_turn[1, pl.ds(t, 1), :]
    cosine[...] = span_cos * row_turn[0] - span_sin * row_turn[1]
    sine[...] = span_sin * row_turn[0] + span_cos * row_turn[1]

    for i in range(2):

        @pl.when(t > 0)
        def _(i=i):
            up[i].wait_recv()

        @pl.when(t < spans - 1)
        def _(i=i):
            down[i].wait_recv()

        both = pl.ds(2 * i * per_frame, 2 * per_frame)
        project_values(halo.at[both], halo_values)

        @pl.loop(0, AH)
        def _(head, i=i):
            cols = pl.ds(pl.multiple_of(head * HD, HD), HD)
            partial[:, cols] = partial[:, cols] + sample(halo_values, (-1 - i, frames + i), head)

        if i == 0:
            loads[3].wait()
            for _ in wo_gather.arrivals():
                pass


    def rows_of(k, which):
        return pl.ds(pl.multiple_of(k * size + which * part, part), part)

    rs = []
    for k in range(chunks):
        rs_send[k] = partial[rows_of(k, 1 - core), :].astype(BF)
        rs.append(remote(rs_send.at[k], rs_recv.at[k], rs_ss.at[k], rs_rs.at[k], {"mp": partner}))
        rs[k].start()
    exchange = []
    for k in range(chunks):
        rs[k].wait_recv()
        ex[chip, k] = (partial[rows_of(k, core), :] + rs_recv[k].astype(F32)).astype(BF)
        copies = []
        for d in range(1, chips):
            mine = ex.at[chip, k]
            copies.append(
                remote(mine, mine, ex_ss.at[k, d], ex_rs.at[k, d], {"mp": (chip + d) % chips * 2 + core})
            )
            copies[-1].start()
        exchange.append(copies)
    loads[5].wait()

    def chunk_slice(k):
        return slice(k * size, (k + 1) * size)

    vx_gathers, ab_copies, sq = [], [], []
    for k in range(chunks):
        for copy in exchange[k]:
            copy.wait_recv()
        total = ex[0, k].astype(F32)
        for c in range(1, chips):
            total = total + ex[c, k].astype(F32)
        mixed = jnp.dot(total.astype(BF), wo[...].reshape(width, width), preferred_element_type=F32)
        ab[k, core] = (queries[rows_of(k, core), :].astype(F32) + mixed).astype(BF)
        mine = ab.at[k, core]
        ab_copies.append(remote(mine, mine, ab_ss.at[k], ab_rs.at[k], {"mp": partner}))
        ab_copies[k].start()
        ab_copies[k].wait_recv()
        visual = jnp.dot(ab[k].reshape(size, width), wp[...], preferred_element_type=F32)
        vx[me, chunk_slice(k), :] = (visual * flat(gain)).astype(BF)
        squares = jnp.broadcast_to(jnp.sum(visual * visual, axis=1, keepdims=True), (size, HD)).T
        ssq[k, 0] = squares[0:8]
        for d in range(1, groups):
            copy = remote(
                ssq.at[k, 0], ssq.at[k, d], sq_ss.at[k, d], sq_rs.at[k, d], {"mp": (me + d) % groups}
            )
            copy.start()
            sq.append(copy)
        gather = Gather(
            lambda s, k=k: vx.at[s, pl.ds(k * size, size)],
            vx.at[me, pl.ds(k * size, size)],
            gather_sems(1 + k),
            groups,
            me,
        )
        gather.start()
        vx_gathers.append(gather)

    tile = 256 if q_width % 256 == 0 else 128

    def slot_rows(slot):
        return pl.ds(pl.multiple_of(slot * model, 64), model)

    def add_cache(slot, span, first):
        term = jnp.dot(vx[slot, span, :], wc[slot_rows(slot), :], preferred_element_type=F32)
        kv_acc[span, :] = term if first else kv_acc[span, :] + term

    def add_query(slot, span, first):
        for c in range(q_width // tile):
            cols = slice(c * tile, (c + 1) * tile)
            term = jnp.dot(vx[slot, span, :], wq[slot_rows(slot), cols], preferred_element_type=F32)
            q_acc[span, cols] = term if first else q_acc[span, cols] + term

    def turn(x, cos, sin):
        return x * cos + pltpu.roll(x, HD // 2, 1) * sin

    def finish_cache(k):
        span = chunk_slice(k)
        square_sum = ssq[k, 0]
        for d in range(1, groups):
            sq[k * (groups - 1) + d - 1].wait_recv()
            square_sum = square_sum + ssq[k, d]
        scale_row = lax.rsqrt(square_sum * (1.0 / (model * groups)) + epsilon)
        scale[span, :] = jnp.broadcast_to(scale_row[0:1], (HD, size)).T
        bias = flat(cache_bias)
        for i in range(ch):
            is_key = me * ch + i < KVH
            cols = slice(i * HD, (i + 1) * HD)
            state = kv_acc[span, cols] * scale[span, :] + bias[:, cols]
            cos = jnp.where(is_key, cosine[span, :], 1.0)
            sin = jnp.where(is_key, sine[span, :], 0.0)
            state = turn(state, cos, sin).astype(BF)
            kv[t, me, span, cols] = state
            key_value[span, cols] = state

    def finish_query(k):
        span = chunk_slice(k)
        bias = flat(query_bias)
        for i in range(q_heads):
            cols = slice(i * HD, (i + 1) * HD)
            state = q_acc[span, cols] * scale[span, :] + bias[:, cols]
            qs[i, span, :] = turn(state, cosine[span, :], sine[span, :]).astype(BF)

    table = shared_heads(groups, q_heads, ch)

    def share_copy(d, k, entry):
        source, target, first, count = entry
        block = kv.at[
            lax.rem(t + spans - d, spans), source, pl.ds(k * size, size), pl.ds(first * HD, count * HD)
        ]
        return remote(block, block, d_ss.at[d, k, target], d_rs.at[d, k, source], {"mp": target})

    def share(d, k):
        for entry in table:

            @pl.when(me == entry[0])
            def _(entry=entry):
                share_copy(d, k, entry).start()

    def share_wait(d, k):
        for entry in table:

            @pl.when(me == entry[1])
            def _(entry=entry):
                share_copy(d, k, entry).wait_recv()

    def share_drain(d, k):
        for entry in table:

            @pl.when(me == entry[0])
            def _(entry=entry):
                share_copy(d, k, entry).wait_send()

    def pass_copy(d, k):
        block = kv.at[lax.rem(t + spans - d, spans), me, pl.ds(k * size, size)]
        return remote(block, block, z_ss.at[d, k], z_rs.at[d + 1, k], {"tm": (t + 1) % spans})

    def arrive_copy(d, k):
        block = kv.at[lax.rem(t + spans - d, spans), me, pl.ds(k * size, size)]
        return remote(block, block, z_ss.at[d, k], z_rs.at[d, k], {"tm": (t + spans - 1) % spans})

    def hand_on(d, k):
        @pl.when(t < spans - 1)
        def _():
            pass_copy(d, k).start()

        share(d, k)

    def service(d, k):
        arrive_copy(d, k).wait_recv()
        hand_on(d, k)

    loads[6].wait()
    loads[7].wait()
    everything = slice(0, rows)
    add_cache(me, everything, True)
    add_query(me, everything, True)
    arrivals = [gather.arrivals() for gather in vx_gathers]
    for k in range(chunks):
        slot = next(arrivals[k])
    add_cache(slot, everything, False)
    add_query(slot, everything, False)
    for k in range(chunks):
        span = chunk_slice(k)
        slots = []
        for slot in arrivals[k]:
            add_cache(slot, span, False)
            slots.append(slot)
        finish_cache(k)
        hand_on(0, k)
        for slot in slots:
            add_query(slot, span, False)
        finish_query(k)
        if k == 0 and chunks > 1:

            @pl.when(t > 0)
            def _():
                service(1, 0)

    def service_all(d):
        for k in range(chunks):
            if k == 0 and chunks > 1:

                @pl.when(d > 1)
                def _():
                    service(d, 0)
            else:
                service(d, k)

    def attend(d, diagonal):
        j = lax.rem(t + spans - d, spans)

        @pl.loop(0, q_heads, unroll=3 if q_heads % 3 == 0 else 1)
        def _(i):
            g = (me * q_heads + i) // GROUP
            k_cols = pl.ds(pl.multiple_of(lax.rem(g, ch) * HD, HD), HD)
            keys = kv[j, g // ch, :, k_cols]
            values = kv[j, (KVH + g) // ch, :, pl.ds(pl.multiple_of(lax.rem(KVH + g, ch) * HD, HD), HD)]
            scores = lax.dot_general(
                qs[i], keys, (((1,), (1,)), ((), ())), preferred_element_type=F32
            ) * (HD ** -0.5 * 1.4426950408889634)
            if diagonal:
                q_pos = lax.broadcasted_iota(jnp.int32, (rows, rows), 0)
                k_pos = lax.broadcasted_iota(jnp.int32, (rows, rows), 1)
                scores = jnp.where(k_pos <= q_pos, scores, masked)
            top = jnp.max(scores, axis=1, keepdims=True)
            if diagonal:
                new_peak = jnp.broadcast_to(top, (rows, HD))
            else:
                new_peak = jnp.maximum(peak[i], top)
            weights = jnp.exp2(scores - new_peak[:, 0:1])
            added = jnp.sum(weights, axis=1, keepdims=True)
            product = jnp.dot(weights.astype(BF), values, preferred_element_type=F32)
            if diagonal:
                denom[i] = jnp.broadcast_to(added, (rows, HD))
                numer[i] = product
            else:
                rescale = jnp.exp2(peak[i] - new_peak)
                denom[i] = denom[i] * rescale + added
                numer[i] = numer[i] * rescale + product
            peak[i] = new_peak

    def share_wait_all(d):
        for k in range(chunks):
            share_wait(d, k)

    last = t == spans - 1

    @pl.when(t < spans - 1)
    def _():
        @pl.loop(1, t + 1)
        def _(d):
            service_all(d)

    @pl.when(last)
    def _():
        service_all(1)

    share_wait_all(0)
    attend(0, True)

    @pl.loop(1, t + 1)
    def _(d):
        @pl.when(last & (d < t))
        def _():
            service_all(d + 1)

        share_wait_all(d)
        attend(d, False)

    for i in range(q_heads):
        attention[:, i * HD : (i + 1) * HD] = (numer[i] / denom[i]).astype(BF)


    @pl.when(t < spans - 1)
    def _():
        for copy in up:
            copy.wait_send()

        @pl.loop(0, t + 1)
        def _(d):
            for k in range(chunks):
                pass_copy(d, k).wait_send()

    @pl.when(t > 0)
    def _():
        for copy in down:
            copy.wait_send()

    @pl.loop(0, t + 1)
    def _(d):
        for k in range(chunks):
            share_drain(d, k)

    wo_gather.drain()
    for gather in vx_gathers:
        gather.drain()
    for copy in rs + ab_copies + sq:
        copy.wait_send()
    for copies in exchange:
        for copy in copies:
            copy.wait_send()


def rows_first(x):
    return x.reshape(-1, HD) if x.shape[0] % HD == 0 else x[None]


def local(
    features,
    queries,
    anchor_frame,
    anchor_patch,
    time_offset,
    space_offset,
    value_weight,
    point_weight,
    point_bias,
    output_weight,
    project_weight,
    norm_gain,
    query_weight,
    query_bias,
    cache_weight,
    cache_bias,
):
    groups = lax.axis_size("mp")
    spans = lax.axis_size("tm")
    frames_here, patches_here, width = features.shape
    cells = frames_here * patches_here
    rows = queries.shape[0]
    chunks = max(1, rows // chunk_rows)
    size = rows // chunks
    part = size // 2
    frequency = rope_base ** (-2.0 * np.arange(HD // 2, dtype=np.float64) / HD)
    sign = np.concatenate([-np.ones(HD // 2), np.ones(HD // 2)])

    def turns(positions):
        angles = positions[:, None] * np.concatenate([frequency, frequency])[None, :]
        return jnp.asarray(np.stack([np.cos(angles), np.sin(angles) * sign]).astype(np.float32))

    row_turn = turns(np.arange(rows, dtype=np.float64))
    span_turn = turns(np.arange(spans, dtype=np.float64) * rows)
    model = project_weight.shape[1]
    q_width = query_weight.shape[1]
    c_width = cache_weight.shape[1]
    q_heads = q_width // HD
    chips = groups // 2
    vmem = pl.BlockSpec(memory_space=pltpu.VMEM)
    hbm = pl.BlockSpec(memory_space=pltpu.HBM)
    dma = pltpu.SemaphoreType.DMA
    V = pltpu.VMEM
    return tuple(
        pl.pallas_call(
            functools.partial(kernel, groups, spans, frames_here, chunks),
            out_shape=(
                jax.ShapeDtypeStruct((rows, q_width), BF),
                jax.ShapeDtypeStruct((rows, c_width), BF),
            ),
            in_specs=[hbm] * 3 + [vmem] * 10 + [hbm] * 5,
            out_specs=(vmem, vmem),
            scratch_shapes=[
                V((cells, width), BF),
                V((rows, width), BF),
                V((2, rows, HD), F32),
                V((width, width), BF),
                V((groups, width // groups, width), BF),
                V((width, model), BF),
                V(query_weight.shape, BF),
                V(cache_weight.shape, BF),
                V((4 * patches_here, width), BF),
                V((cells, width), BF),
                V((2 * patches_here, width), BF),
                V((rows, HD), F32),
                V((AH, 4 * POINTS, rows), F32),
                V((rows, HD), F32),
                V((rows, HD), F32),
                V((max(2, frames_here) * patches_here, rows), F32),
                V((rows, width), F32),
                V((chunks, part, width), BF),
                V((chunks, part, width), BF),
                V((chips, chunks, part, width), BF),
                V((chunks, 2, part, width), BF),
                V((groups, rows, model), BF),
                V((chunks, groups, 8, size), F32),
                V((rows, HD), F32),
                V((rows, q_width), F32),
                V((rows, c_width), F32),
                V((q_heads, rows, HD), BF),
                V((spans, groups, rows, c_width), BF),
                V((q_heads, rows, HD), F32),
                V((q_heads, rows, HD), F32),
                V((q_heads, rows, HD), F32),
                dma((8,)),
                dma((2, 2)),
                dma((2, 2)),
                dma((chunks,)),
                dma((chunks,)),
                dma((chunks, chips)),
                dma((chunks, chips)),
                dma((chunks,)),
                dma((chunks,)),
                dma((chunks, groups)),
                dma((chunks, groups)),
                dma((spans, chunks)),
                dma((spans, chunks)),
                dma((spans, chunks, groups)),
                dma((spans, chunks, groups)),
                dma((1 + chunks, 4, chips)),
            ],
            compiler_params=pltpu.CompilerParams(
                collective_id=0, has_side_effects=True, vmem_limit_bytes=48 * 1024 * 1024
            ),
        )(
            *[
                pltpu.with_memory_space_constraint(x, pltpu.HBM)
                for x in (
                    features.reshape(cells, width),
                    queries,
                    row_turn,
                    anchor_frame[None],
                    anchor_patch[None],
                    time_offset.transpose(1, 2, 0),
                    space_offset.transpose(0, 2, 3, 1),
                    point_weight.T,
                    point_bias[None],
                    span_turn,
                    rows_first(norm_gain),
                    rows_first(query_bias),
                    rows_first(cache_bias),
                    value_weight,
                    output_weight,
                    project_weight,
                    query_weight,
                    cache_weight,
                )
            ]
        )
    )


def solution(mesh):
    return jax.shard_map(
        local,
        mesh=mesh,
        in_specs=(
            P(("dp", "tm"), "mp", None),
            P(("dp", "tm"), None),
            P(("dp", "tm")),
            P(("dp", "tm")),
            P(("dp", "tm"), None, None),
            P(None, ("dp", "tm"), None, None),
            P(),
            P(),
            P(),
            P("mp", None),
            P(None, "mp"),
            P("mp"),
            P(None, "mp"),
            P("mp"),
            P(None, "mp"),
            P("mp"),
        ),
        out_specs=(P(("dp", "tm"), "mp"), P(("dp", "tm"), "mp")),
        check_vma=False,
    )
```

```python
import functools

import jax
import jax.numpy as jnp
import numpy as np
from jax import lax
from jax.experimental import pallas as pl
from jax.experimental.pallas import tpu as pltpu
from jax.sharding import PartitionSpec as P

AH = 8
POINTS = 4
GRID = 24
KVH = 4
HD = 128
GROUP = 7

rope_base = 1000000.0
epsilon = 1e-06
masked = -1e30
chunk_rows = 64
MESH = pl.DeviceIdType.MESH
BF = jnp.bfloat16
F32 = jnp.float32


def remote(src, dst, send, recv, device):
    return pltpu.make_async_remote_copy(
        src_ref=src, dst_ref=dst, send_sem=send, recv_sem=recv, device_id=device, device_id_type=MESH
    )


class Gather:
    def __init__(self, slot_ref, own, sems, groups, me):
        self.chips = groups // 2
        self.chip, self.core = me // 2, me % 2
        self.me, self.partner = me, me + 1 - 2 * (me % 2)
        cs, cr, ps, pr = sems
        self.cross = [None] + [
            remote(
                own,
                slot_ref(me),
                cs(d),
                cr(d),
                {"mp": (self.chip + d) % self.chips * 2 + self.core},
            )
            for d in range(1, self.chips)
        ]
        self.near = [remote(own, slot_ref(me), ps(0), pr(0), {"mp": self.partner})]
        for d in range(1, self.chips):
            slot = slot_ref(self.slot(d, self.core))
            self.near.append(remote(slot, slot, ps(d), pr(d), {"mp": self.partner}))

    def slot(self, d, core):
        return (self.chip + self.chips - d) % self.chips * 2 + core

    def start(self):
        for copy in self.cross[1:]:
            copy.start()
        self.near[0].start()

    def arrivals(self):
        self.near[0].wait_recv()
        yield self.partner
        for d in range(1, self.chips):
            self.cross[d].wait_recv()
            self.near[d].start()
            yield self.slot(d, self.core)
            self.near[d].wait_recv()
            yield self.slot(d, 1 - self.core)

    def drain(self):
        for copy in self.cross[1:] + self.near:
            copy.wait_send()


def shared_heads(groups, q_heads, ch):
    table = []
    for source in range(groups):
        for target in range(groups):
            wanted = {(target * q_heads + i) // GROUP for i in range(q_heads)}
            need = [h for h in range(ch) if (source * ch + h) % KVH in wanted]
            if target != source and need:
                table.append((source, target, need[0], need[-1] - need[0] + 1))
    return table


def flat(ref):
    return jnp.concatenate([ref[i : i + 1, :] for i in range(ref.shape[0])], axis=1)


def kernel(
    groups,
    spans,
    frames,
    chunks,
    features,
    queries_hbm,
    row_turn_hbm,
    anchor_frame,
    anchor_patch,
    time_offset,
    space_offset,
    point_weight,
    point_bias,
    span_turn,
    gain,
    query_bias,
    cache_bias,
    value_hbm,
    output_hbm,
    project_hbm,
    query_hbm,
    cache_hbm,
    attention,
    key_value,
    own_features,
    queries,
    row_turn,
    vw,
    wo,
    wp,
    wq,
    wc,
    halo,
    own_values,
    halo_values,
    logits,
    coords,
    cosine,
    sine,
    vw_turned,
    sums,
    partial,
    rs_send,
    rs_recv,
    ex,
    ab,
    vx,
    ssq,
    scale,
    q_acc,
    kv_acc,
    qs,
    kv,
    peak,
    denom,
    numer,
    load_sem,
    halo_ss,
    halo_rs,
    rs_ss,
    rs_rs,
    ex_ss,
    ex_rs,
    ab_ss,
    ab_rs,
    sq_ss,
    sq_rs,
    z_ss,
    z_rs,
    d_ss,
    d_rs,
    ag_sem,
):
    me = lax.axis_index("mp")
    t = lax.axis_index("tm")
    cells, width = features.shape
    rows = queries.shape[0]
    per_frame = cells // frames
    lines = per_frame // GRID
    model = wp.shape[1]
    q_width = wq.shape[1]
    q_heads = qs.shape[0]
    ch = kv.shape[3] // HD
    chips = groups // 2
    chip, core = me // 2, me % 2
    partner = me + 1 - 2 * core
    size = rows // chunks
    part = size // 2
    padded = ssq.shape[3]

    barrier = pltpu.get_barrier_semaphore()
    for d in range(1, groups):
        pl.semaphore_signal(barrier, inc=1, device_id={"mp": (me + d) % groups}, device_id_type=MESH)

    @pl.when(t < spans - 1)
    def _():
        pl.semaphore_signal(barrier, inc=1, device_id={"tm": (t + 1) % spans}, device_id_type=MESH)

    @pl.when(t > 0)
    def _():
        pl.semaphore_signal(barrier, inc=1, device_id={"tm": (t + spans - 1) % spans}, device_id_type=MESH)

    loads = [
        pltpu.make_async_copy(src, dst, load_sem.at[i])
        for i, (src, dst) in enumerate(
            [
                (queries_hbm, queries),
                (features, own_features),
                (value_hbm, vw),
                (output_hbm, wo.at[me]),
                (row_turn_hbm, row_turn),
                (project_hbm, wp),
                (cache_hbm, wc),
                (query_hbm, wq),
            ]
        )
    ]
    for load in loads:
        load.start()

    neighbours = jnp.where(t > 0, 1, 0) + jnp.where(t < spans - 1, 1, 0)
    pl.semaphore_wait(barrier, groups - 1 + neighbours)

    up, down = [], []
    for i in range(2):
        up.append(
            remote(
                features.at[pl.ds((frames - 1 - i) * per_frame, per_frame)],
                halo.at[pl.ds(2 * i * per_frame, per_frame)],
                halo_ss.at[0, i],
                halo_rs.at[0, i],
                {"tm": (t + 1) % spans},
            )
        )
        down.append(
            remote(
                features.at[pl.ds(i * per_frame, per_frame)],
                halo.at[pl.ds((2 * i + 1) * per_frame, per_frame)],
                halo_ss.at[1, i],
                halo_rs.at[1, i],
                {"tm": (t + spans - 1) % spans},
            )
        )

    @pl.when(t < spans - 1)
    def _():
        for copy in up:
            copy.start()

    @pl.when(t > 0)
    def _():
        for copy in down:
            copy.start()

    def gather_sems(index):
        return [functools.partial(lambda k, d: ag_sem.at[index, k, d], k) for k in range(4)]

    wo_gather = Gather(lambda s: wo.at[s], output_hbm, gather_sems(0), groups, me)
    wo_gather.start()

    @pl.when(t == 0)
    def _():
        for i in range(2):
            halo[pl.ds(2 * i * per_frame, per_frame), :] = jnp.zeros((per_frame, width), BF)

    @pl.when(t == spans - 1)
    def _():
        for i in range(2):
            halo[pl.ds((2 * i + 1) * per_frame, per_frame), :] = jnp.zeros((per_frame, width), BF)

    loads[0].wait()
    logits[...] = jnp.zeros((rows, HD), F32)
    logits[:, 0 : AH * POINTS] = (
        lax.dot_general(
            queries[...], point_weight[...], (((1,), (1,)), ((), ())), preferred_element_type=F32
        )
        + point_bias[...]
    )
    by_point = logits[...].T
    frame_at = anchor_frame[...].astype(F32)
    patch = anchor_patch[...].astype(F32)
    row_at = jnp.floor((patch + 0.5) * (1.0 / GRID))
    column_at = patch - row_at * GRID
    for h in range(AH):
        own = by_point[h * POINTS : (h + 1) * POINTS]
        own = jnp.exp(own - jnp.max(own, axis=0, keepdims=True))
        coords[h, 0:4, :] = time_offset[h] + frame_at
        coords[h, 4:8, :] = space_offset[0, h] + row_at
        coords[h, 8:12, :] = space_offset[1, h] + column_at
        coords[h, 12:16, :] = own / jnp.sum(own, axis=0, keepdims=True)

    loads[1].wait()
    loads[2].wait()

    def project_values(source, target):
        for c in range(width // 256):
            columns = slice(c * 256, (c + 1) * 256)
            target[columns, :] = lax.dot_general(
                vw_turned[columns, :], source[...], (((1,), (1,)), ((), ())), preferred_element_type=F32
            ).astype(BF)

    line_index = lax.broadcasted_iota(jnp.int32, (GRID, rows), 0).astype(F32)
    first_line = (me * lines).astype(F32)
    first_frame = (t * frames).astype(F32)

    def hat(position, cell):
        return jnp.maximum(1.0 - jnp.abs(position - cell), 0.0)

    def sample(values, offsets, head):
        info = coords[head]
        columns = [hat(info[8 + k : 9 + k], line_index) for k in range(POINTS)]
        blocks = []
        for offset in offsets:
            timed = info[12:16] * hat(info[0:4], first_frame + offset)
            for line in range(lines):
                share = timed * hat(info[4:8], first_line + line)
                total = share[0:1] * columns[0]
                for k in range(1, POINTS):
                    total = total + share[k : k + 1] * columns[k]
                blocks.append(total)
        corner = jnp.concatenate(blocks, axis=0).astype(BF)
        mine = values[pl.ds(pl.multiple_of(head * HD, HD), HD), :]
        return jnp.dot(mine, corner, preferred_element_type=F32)

    for c in range(width // 256):
        columns = slice(c * 256, (c + 1) * 256)
        vw_turned[columns, :] = vw[:, columns].T
    project_values(own_features, own_values)


    @pl.loop(0, AH, unroll=2)
    def _(head):
        sums[pl.ds(pl.multiple_of(head * HD, HD), HD), :] = sample(own_values, range(frames), head)

    loads[4].wait()
    span_cos, span_sin = span_turn[0, pl.ds(t, 1), :], span_turn[1, pl.ds(t, 1), :]
    cosine[...] = span_cos * row_turn[0] - span_sin * row_turn[1]
    sine[...] = span_sin * row_turn[0] + span_cos * row_turn[1]

    for i in range(2):

        @pl.when(t > 0)
        def _(i=i):
            up[i].wait_recv()

        @pl.when(t < spans - 1)
        def _(i=i):
            down[i].wait_recv()

        both = pl.ds(2 * i * per_frame, 2 * per_frame)
        if i == 1:
            loads[3].wait()
            wo_arrivals = wo_gather.arrivals()
            for _ in range(2 * chips - 2):
                next(wo_arrivals)
        project_values(halo.at[both], halo_values)

        @pl.loop(0, AH, unroll=2)
        def _(head, i=i):
            mine = pl.ds(pl.multiple_of(head * HD, HD), HD)
            total = sums[mine, :] + sample(halo_values, (-1 - i, frames + i), head)
            if i == 0:
                sums[mine, :] = total
            else:
                partial[:, mine] = total.T


    def part_rows(k, which):
        return pl.ds(pl.multiple_of(k * size + which * part, part), part)

    def chunk_rows_of(k):
        return pl.ds(k * size, size)

    rs = []
    for k in range(chunks):
        rs_send[k] = partial[part_rows(k, 1 - core), :].astype(BF)
        rs.append(remote(rs_send.at[k], rs_recv.at[k], rs_ss.at[k], rs_rs.at[k], {"mp": partner}))
        rs[k].start()
    exchange = []
    for k in range(chunks):
        rs[k].wait_recv()
        ex[chip, k] = (partial[part_rows(k, core), :] + rs_recv[k].astype(F32)).astype(BF)
        copies = []
        for d in range(1, chips):
            mine = ex.at[chip, k]
            copies.append(
                remote(mine, mine, ex_ss.at[k, d], ex_rs.at[k, d], {"mp": (chip + d) % chips * 2 + core})
            )
            copies[-1].start()
        exchange.append(copies)
    loads[5].wait()
    for _ in wo_arrivals:
        pass

    def chunk_slice(k):
        return slice(k * size, (k + 1) * size)

    vx_gathers, ab_copies, sq = [], [], []

    def mix(k):
        for copy in exchange[k]:
            copy.wait_recv()
        total = ex[0, k].astype(F32)
        for c in range(1, chips):
            total = total + ex[c, k].astype(F32)
        mixed = jnp.dot(total.astype(BF), wo[...].reshape(width, width), preferred_element_type=F32)
        ab[k, core] = (queries[part_rows(k, core), :].astype(F32) + mixed).astype(BF)
        mine = ab.at[k, core]
        ab_copies.append(remote(mine, mine, ab_ss.at[k], ab_rs.at[k], {"mp": partner}))
        ab_copies[k].start()

    def project(k):
        ab_copies[k].wait_recv()
        visual = jnp.dot(ab[k].reshape(size, width), wp[...], preferred_element_type=F32)
        vx[me, chunk_slice(k), :] = (visual * flat(gain)).astype(BF)
        gather = Gather(
            lambda s, k=k: vx.at[s, pl.ds(k * size, size)],
            vx.at[me, pl.ds(k * size, size)],
            gather_sems(1 + k),
            groups,
            me,
        )
        squares = jnp.broadcast_to(jnp.sum(visual * visual, axis=1, keepdims=True), (size, HD))
        if padded > size:
            squares = jnp.concatenate([squares, jnp.zeros((padded - size, HD), F32)], axis=0)
        ssq[k, 0] = squares.T[0:8]
        for d in range(1, groups):
            copy = remote(
                ssq.at[k, 0], ssq.at[k, d], sq_ss.at[k, d], sq_rs.at[k, d], {"mp": (me + d) % groups}
            )
            copy.start()
            sq.append(copy)
        gather.start()
        vx_gathers.append(gather)

    for k in range(chunks):
        mix(k)
        project(k)

    tile = 256 if q_width % 256 == 0 else 128

    def slot_rows(slot):
        return pl.ds(pl.multiple_of(slot * model, 64), model)

    def add_cache(slot, span, first):
        term = jnp.dot(vx[slot, span, :], wc[slot_rows(slot), :], preferred_element_type=F32)
        kv_acc[span, :] = term if first else kv_acc[span, :] + term

    def add_query(slot, span, first):
        for c in range(q_width // tile):
            cols = slice(c * tile, (c + 1) * tile)
            term = jnp.dot(vx[slot, span, :], wq[slot_rows(slot), cols], preferred_element_type=F32)
            q_acc[span, cols] = term if first else q_acc[span, cols] + term

    def turn(x, cos, sin):
        return x * cos + pltpu.roll(x, HD // 2, 1) * sin

    def finish_cache(k):
        span = chunk_slice(k)
        square_sum = ssq[k, 0]
        for d in range(1, groups):
            sq[k * (groups - 1) + d - 1].wait_recv()
            square_sum = square_sum + ssq[k, d]
        scale_row = lax.rsqrt(square_sum * (1.0 / (model * groups)) + epsilon)
        scale[span, :] = jnp.broadcast_to(scale_row[0:1], (HD, padded)).T[0:size]
        bias = flat(cache_bias)
        for i in range(ch):
            is_key = me * ch + i < KVH
            cols = slice(i * HD, (i + 1) * HD)
            state = kv_acc[span, cols] * scale[span, :] + bias[:, cols]
            cos = jnp.where(is_key, cosine[span, :], 1.0)
            sin = jnp.where(is_key, sine[span, :], 0.0)
            state = turn(state, cos, sin).astype(BF)
            kv[t, me, span, cols] = state
            key_value[span, cols] = state

    def finish_query(k):
        span = chunk_slice(k)
        bias = flat(query_bias)
        for i in range(q_heads):
            cols = slice(i * HD, (i + 1) * HD)
            state = q_acc[span, cols] * scale[span, :] + bias[:, cols]
            qs[i, span, :] = turn(state, cosine[span, :], sine[span, :]).astype(BF)

    table = shared_heads(groups, q_heads, ch)

    def share_copy(d, k, entry):
        source, target, first, count = entry
        block = kv.at[
            lax.rem(t + spans - d, spans), source, pl.ds(k * size, size), pl.ds(first * HD, count * HD)
        ]
        return remote(block, block, d_ss.at[d, k, target], d_rs.at[d, k, source], {"mp": target})

    def share(d, k):
        for entry in table:

            @pl.when(me == entry[0])
            def _(entry=entry):
                share_copy(d, k, entry).start()

    def share_wait(d, k):
        for entry in table:

            @pl.when(me == entry[1])
            def _(entry=entry):
                share_copy(d, k, entry).wait_recv()

    def share_drain(d, k):
        for entry in table:

            @pl.when(me == entry[0])
            def _(entry=entry):
                share_copy(d, k, entry).wait_send()

    def pass_copy(d, k):
        block = kv.at[lax.rem(t + spans - d, spans), me, pl.ds(k * size, size)]
        return remote(block, block, z_ss.at[d, k], z_rs.at[d + 1, k], {"tm": (t + 1) % spans})

    def arrive_copy(d, k):
        block = kv.at[lax.rem(t + spans - d, spans), me, pl.ds(k * size, size)]
        return remote(block, block, z_ss.at[d, k], z_rs.at[d, k], {"tm": (t + spans - 1) % spans})

    def hand_on(d, k):
        @pl.when(t < spans - 1)
        def _():
            pass_copy(d, k).start()

        share(d, k)

    def service(d, k):
        arrive_copy(d, k).wait_recv()
        hand_on(d, k)

    loads[6].wait()
    loads[7].wait()
    everything = slice(0, rows)
    add_cache(me, everything, True)
    add_query(me, everything, True)
    arrivals = [gather.arrivals() for gather in vx_gathers]
    for k in range(chunks):
        slot = next(arrivals[k])
    add_cache(slot, everything, False)
    add_query(slot, everything, False)
    for k in range(chunks):
        span = chunk_slice(k)
        slots = []
        for slot in arrivals[k]:
            add_cache(slot, span, False)
            slots.append(slot)
        finish_cache(k)
        hand_on(0, k)
        for slot in slots:
            add_query(slot, span, False)
        finish_query(k)
        for d in range(1, min(k, spans - 1) + 1):

            @pl.when(t >= d)
            def _(d=d, k=k):
                service(d, k - d)

    def wave(w):
        for k in range(chunks):
            d = w - k

            @pl.when((d >= 1) & (d <= t))
            def _(d=d, k=k):
                service(d, k)

    def attend(d, diagonal):
        j = lax.rem(t + spans - d, spans)

        @pl.loop(0, q_heads, unroll=3 if q_heads % 3 == 0 else 1)
        def _(i):
            g = (me * q_heads + i) // GROUP
            k_cols = pl.ds(pl.multiple_of(lax.rem(g, ch) * HD, HD), HD)
            keys = kv[j, g // ch, :, k_cols]
            values = kv[j, (KVH + g) // ch, :, pl.ds(pl.multiple_of(lax.rem(KVH + g, ch) * HD, HD), HD)]
            scores = lax.dot_general(
                qs[i], keys, (((1,), (1,)), ((), ())), preferred_element_type=F32
            ) * (HD ** -0.5 * 1.4426950408889634)
            if diagonal:
                q_pos = lax.broadcasted_iota(jnp.int32, (rows, rows), 0)
                k_pos = lax.broadcasted_iota(jnp.int32, (rows, rows), 1)
                scores = jnp.where(k_pos <= q_pos, scores, masked)
            top = jnp.max(scores, axis=1, keepdims=True)
            if diagonal:
                new_peak = jnp.broadcast_to(top, (rows, HD))
            else:
                new_peak = jnp.maximum(peak[i], top)
            weights = jnp.exp2(scores - new_peak[:, 0:1])
            added = jnp.sum(weights, axis=1, keepdims=True)
            product = jnp.dot(weights.astype(BF), values, preferred_element_type=F32)
            if diagonal:
                denom[i] = jnp.broadcast_to(added, (rows, HD))
                numer[i] = product
            else:
                rescale = jnp.exp2(peak[i] - new_peak)
                denom[i] = denom[i] * rescale + added
                numer[i] = numer[i] * rescale + product
            peak[i] = new_peak

    def share_wait_all(d):
        for k in range(chunks):
            share_wait(d, k)

    last = t == spans - 1

    @pl.when(t < spans - 1)
    def _():
        @pl.loop(chunks, chunks + t)
        def _(w):
            wave(w)

    @pl.when(last & (t > 0))
    def _():
        wave(chunks)

    share_wait_all(0)
    attend(0, True)

    @pl.loop(1, t + 1)
    def _(d):
        @pl.when(last & (d < t))
        def _():
            wave(chunks + d)

        share_wait_all(d)
        attend(d, False)

    for i in range(q_heads):
        attention[:, i * HD : (i + 1) * HD] = (numer[i] / denom[i]).astype(BF)


    @pl.when(t < spans - 1)
    def _():
        for copy in up:
            copy.wait_send()

        @pl.loop(0, t + 1)
        def _(d):
            for k in range(chunks):
                pass_copy(d, k).wait_send()

    @pl.when(t > 0)
    def _():
        for copy in down:
            copy.wait_send()

    @pl.loop(0, t + 1)
    def _(d):
        for k in range(chunks):
            share_drain(d, k)

    wo_gather.drain()
    for gather in vx_gathers:
        gather.drain()
    for copy in rs + ab_copies + sq:
        copy.wait_send()
    for copies in exchange:
        for copy in copies:
            copy.wait_send()


def rows_first(x):
    return x.reshape(-1, HD) if x.shape[0] % HD == 0 else x[None]


def local(
    features,
    queries,
    anchor_frame,
    anchor_patch,
    time_offset,
    space_offset,
    value_weight,
    point_weight,
    point_bias,
    output_weight,
    project_weight,
    norm_gain,
    query_weight,
    query_bias,
    cache_weight,
    cache_bias,
):
    groups = lax.axis_size("mp")
    spans = lax.axis_size("tm")
    frames_here, patches_here, width = features.shape
    cells = frames_here * patches_here
    rows = queries.shape[0]
    chunks = max(1, rows // chunk_rows)
    size = rows // chunks
    part = size // 2
    frequency = rope_base ** (-2.0 * np.arange(HD // 2, dtype=np.float64) / HD)
    sign = np.concatenate([-np.ones(HD // 2), np.ones(HD // 2)])

    def turns(positions):
        angles = positions[:, None] * np.concatenate([frequency, frequency])[None, :]
        return jnp.asarray(np.stack([np.cos(angles), np.sin(angles) * sign]).astype(np.float32))

    row_turn = turns(np.arange(rows, dtype=np.float64))
    span_turn = turns(np.arange(spans, dtype=np.float64) * rows)
    model = project_weight.shape[1]
    q_width = query_weight.shape[1]
    c_width = cache_weight.shape[1]
    q_heads = q_width // HD
    chips = groups // 2
    vmem = pl.BlockSpec(memory_space=pltpu.VMEM)
    hbm = pl.BlockSpec(memory_space=pltpu.HBM)
    dma = pltpu.SemaphoreType.DMA
    V = pltpu.VMEM
    return tuple(
        pl.pallas_call(
            functools.partial(kernel, groups, spans, frames_here, chunks),
            out_shape=(
                jax.ShapeDtypeStruct((rows, q_width), BF),
                jax.ShapeDtypeStruct((rows, c_width), BF),
            ),
            in_specs=[hbm] * 3 + [vmem] * 10 + [hbm] * 5,
            out_specs=(vmem, vmem),
            scratch_shapes=[
                V((cells, width), BF),
                V((rows, width), BF),
                V((2, rows, HD), F32),
                V((width, width), BF),
                V((groups, width // groups, width), BF),
                V((width, model), BF),
                V(query_weight.shape, BF),
                V(cache_weight.shape, BF),
                V((4 * patches_here, width), BF),
                V((width, cells), BF),
                V((width, 2 * patches_here), BF),
                V((rows, HD), F32),
                V((AH, 4 * POINTS, rows), F32),
                V((rows, HD), F32),
                V((rows, HD), F32),
                V((width, width), BF),
                V((width, rows), F32),
                V((rows, width), F32),
                V((chunks, part, width), BF),
                V((chunks, part, width), BF),
                V((chips, chunks, part, width), BF),
                V((chunks, 2, part, width), BF),
                V((groups, rows, model), BF),
                V((chunks, groups, 8, -(-size // HD) * HD), F32),
                V((rows, HD), F32),
                V((rows, q_width), F32),
                V((rows, c_width), F32),
                V((q_heads, rows, HD), BF),
                V((spans, groups, rows, c_width), BF),
                V((q_heads, rows, HD), F32),
                V((q_heads, rows, HD), F32),
                V((q_heads, rows, HD), F32),
                dma((8,)),
                dma((2, 2)),
                dma((2, 2)),
                dma((chunks,)),
                dma((chunks,)),
                dma((chunks, chips)),
                dma((chunks, chips)),
                dma((chunks,)),
                dma((chunks,)),
                dma((chunks, groups)),
                dma((chunks, groups)),
                dma((spans, chunks)),
                dma((spans, chunks)),
                dma((spans, chunks, groups)),
                dma((spans, chunks, groups)),
                dma((1 + chunks, 4, chips)),
            ],
            compiler_params=pltpu.CompilerParams(
                collective_id=0, has_side_effects=True, vmem_limit_bytes=48 * 1024 * 1024
            ),
        )(
            *[
                pltpu.with_memory_space_constraint(x, pltpu.HBM)
                for x in (
                    features.reshape(cells, width),
                    queries,
                    row_turn,
                    anchor_frame[None],
                    anchor_patch[None],
                    time_offset.transpose(1, 2, 0),
                    space_offset.transpose(0, 2, 3, 1),
                    point_weight.T,
                    point_bias[None],
                    span_turn,
                    rows_first(norm_gain),
                    rows_first(query_bias),
                    rows_first(cache_bias),
                    value_weight,
                    output_weight,
                    project_weight,
                    query_weight,
                    cache_weight,
                )
            ]
        )
    )


def solution(mesh):
    return jax.shard_map(
        local,
        mesh=mesh,
        in_specs=(
            P(("dp", "tm"), "mp", None),
            P(("dp", "tm"), None),
            P(("dp", "tm")),
            P(("dp", "tm")),
            P(("dp", "tm"), None, None),
            P(None, ("dp", "tm"), None, None),
            P(),
            P(),
            P(),
            P("mp", None),
            P(None, "mp"),
            P("mp"),
            P(None, "mp"),
            P("mp"),
            P(None, "mp"),
            P("mp"),
        ),
        out_specs=(P(("dp", "tm"), "mp"), P(("dp", "tm"), "mp")),
        check_vma=False,
    )
```

```python
import functools

import jax
import jax.numpy as jnp
import numpy as np
from jax import lax
from jax.experimental import pallas as pl
from jax.experimental.pallas import tpu as pltpu
from jax.sharding import PartitionSpec as P

AH = 8
POINTS = 4
GRID = 24
KVH = 4
HD = 128
GROUP = 7

rope_base = 1000000.0
epsilon = 1e-06
masked = -1e30
MESH = pl.DeviceIdType.MESH
BF = jnp.bfloat16
F32 = jnp.float32


def remote(src, dst, send, recv, device):
    return pltpu.make_async_remote_copy(
        src_ref=src, dst_ref=dst, send_sem=send, recv_sem=recv, device_id=device, device_id_type=MESH
    )


class Gather:
    def __init__(self, slot_ref, own, sems, groups, me):
        self.chips = groups // 2
        self.chip, self.core = me // 2, me % 2
        self.me, self.partner = me, me + 1 - 2 * (me % 2)
        cs, cr, ps, pr = sems
        self.cross = [None] + [
            remote(
                own,
                slot_ref(me),
                cs(d),
                cr(d),
                {"mp": (self.chip + d) % self.chips * 2 + self.core},
            )
            for d in range(1, self.chips)
        ]
        self.near = [remote(own, slot_ref(me), ps(0), pr(0), {"mp": self.partner})]
        for d in range(1, self.chips):
            slot = slot_ref(self.slot(d, self.core))
            self.near.append(remote(slot, slot, ps(d), pr(d), {"mp": self.partner}))

    def slot(self, d, core):
        return (self.chip + self.chips - d) % self.chips * 2 + core

    def start(self):
        for copy in self.cross[1:]:
            copy.start()
        self.near[0].start()

    def arrivals(self):
        self.near[0].wait_recv()
        yield self.partner
        for d in range(1, self.chips):
            self.cross[d].wait_recv()
            self.near[d].start()
            yield self.slot(d, self.core)
            self.near[d].wait_recv()
            yield self.slot(d, 1 - self.core)

    def drain(self):
        for copy in self.cross[1:] + self.near:
            copy.wait_send()


def row_chunks(rows):
    return ((0, 3 * rows // 8), (3 * rows // 8, 3 * rows // 8), (3 * rows // 4, rows // 4))


def shared_heads(groups, q_heads, ch):
    table = []
    for source in range(groups):
        for target in range(groups):
            wanted = {(target * q_heads + i) // GROUP for i in range(q_heads)}
            need = [h for h in range(ch) if (source * ch + h) % KVH in wanted]
            if target != source and need:
                sent = sum(e[0] == source for e in table)
                received = sum(e[1] == target for e in table)
                table.append((source, target, need[0], need[-1] - need[0] + 1, sent, received))
    return table


def flat(ref):
    return jnp.concatenate([ref[i : i + 1, :] for i in range(ref.shape[0])], axis=1)


def kernel(
    groups,
    spans,
    frames,
    plan,
    features,
    queries_hbm,
    row_turn_hbm,
    anchor_frame,
    anchor_patch,
    time_offset,
    space_offset,
    point_weight,
    point_bias,
    span_turn,
    gain,
    query_bias,
    cache_bias,
    value_hbm,
    output_hbm,
    project_hbm,
    query_hbm,
    cache_hbm,
    attention_out,
    key_value_out,
    attention,
    key_value,
    own_features,
    queries,
    row_turn,
    vw,
    wo,
    wp,
    wq,
    wc,
    halo,
    own_values,
    halo_values,
    logits,
    coords,
    cosine,
    sine,
    vw_turned,
    sums,
    partial,
    rs_send,
    rs_recv,
    ex,
    ab,
    vx,
    ssq,
    scale,
    q_acc,
    kv_acc,
    qs,
    kv,
    peak,
    denom,
    numer,
    load_sem,
    out_sem,
    halo_ss,
    halo_rs,
    rs_ss,
    rs_rs,
    ex_ss,
    ex_rs,
    ab_ss,
    ab_rs,
    sq_ss,
    sq_rs,
    z_ss,
    z_rs,
    d_ss,
    d_rs,
    ag_sem,
):
    me = lax.axis_index("mp")
    t = lax.axis_index("tm")
    cells, width = features.shape
    rows = queries.shape[0]
    per_frame = cells // frames
    lines = per_frame // GRID
    model = wp.shape[1]
    q_width = wq.shape[1]
    q_heads = qs.shape[0]
    ch = kv.shape[3] // HD
    chips = groups // 2
    chip, core = me // 2, me % 2
    partner = me + 1 - 2 * core
    chunks = len(plan)
    padded = ssq.shape[3]

    barrier = pltpu.get_barrier_semaphore()
    for d in range(1, groups):
        pl.semaphore_signal(barrier, inc=1, device_id={"mp": (me + d) % groups}, device_id_type=MESH)

    for d in range(1, spans):
        pl.semaphore_signal(barrier, inc=1, device_id={"tm": (t + d) % spans}, device_id_type=MESH)

    loads = [
        pltpu.make_async_copy(src, dst, load_sem.at[i])
        for i, (src, dst) in enumerate(
            [
                (queries_hbm, queries),
                (features, own_features),
                (value_hbm, vw),
                (output_hbm, wo.at[me]),
                (row_turn_hbm, row_turn),
                (project_hbm, wp),
                (cache_hbm, wc),
                (query_hbm, wq),
            ]
        )
    ]
    for load in loads:
        load.start()

    pl.semaphore_wait(barrier, groups + spans - 2)

    up, down = [], []
    for i in range(2):
        up.append(
            remote(
                features.at[pl.ds((frames - 1 - i) * per_frame, per_frame)],
                halo.at[pl.ds(2 * i * per_frame, per_frame)],
                halo_ss.at[0, i],
                halo_rs.at[0, i],
                {"tm": (t + 1) % spans},
            )
        )
        down.append(
            remote(
                features.at[pl.ds(i * per_frame, per_frame)],
                halo.at[pl.ds((2 * i + 1) * per_frame, per_frame)],
                halo_ss.at[1, i],
                halo_rs.at[1, i],
                {"tm": (t + spans - 1) % spans},
            )
        )

    @pl.when(t < spans - 1)
    def _():
        for copy in up:
            copy.start()

    @pl.when(t > 0)
    def _():
        for copy in down:
            copy.start()

    def gather_sems(index):
        firsts = (-1, chips - 2, 2 * chips - 2, 3 * chips - 2)
        return [functools.partial(lambda first, d: ag_sem.at[index, first + d], first) for first in firsts]

    wo_gather = Gather(lambda s: wo.at[s], output_hbm, gather_sems(0), groups, me)
    wo_gather.start()

    @pl.when(t == 0)
    def _():
        for i in range(2):
            halo[pl.ds(2 * i * per_frame, per_frame), :] = jnp.zeros((per_frame, width), BF)

    @pl.when(t == spans - 1)
    def _():
        for i in range(2):
            halo[pl.ds((2 * i + 1) * per_frame, per_frame), :] = jnp.zeros((per_frame, width), BF)

    loads[0].wait()
    logits[...] = jnp.zeros((rows, HD), F32)
    logits[:, 0 : AH * POINTS] = (
        lax.dot_general(
            queries[...], point_weight[...], (((1,), (1,)), ((), ())), preferred_element_type=F32
        )
        + point_bias[...]
    )
    by_point = logits[...].T
    frame_at = anchor_frame[...].astype(F32)
    patch = anchor_patch[...].astype(F32)
    row_at = jnp.floor((patch + 0.5) * (1.0 / GRID))
    column_at = patch - row_at * GRID
    for h in range(AH):
        own = by_point[h * POINTS : (h + 1) * POINTS]
        own = jnp.exp(own - jnp.max(own, axis=0, keepdims=True))
        coords[h, 0:4, :] = time_offset[h] + frame_at
        coords[h, 4:8, :] = space_offset[0, h] + row_at
        coords[h, 8:12, :] = space_offset[1, h] + column_at
        coords[h, 12:16, :] = own / jnp.sum(own, axis=0, keepdims=True)

    loads[1].wait()
    loads[2].wait()

    def project_values(source, target):
        for c in range(width // 256):
            columns = slice(c * 256, (c + 1) * 256)
            target[columns, :] = lax.dot_general(
                vw_turned[columns, :], source[...], (((1,), (1,)), ((), ())), preferred_element_type=F32
            ).astype(BF)

    line_index = lax.broadcasted_iota(jnp.int32, (GRID, rows), 0).astype(F32)
    first_line = (me * lines).astype(F32)
    first_frame = (t * frames).astype(F32)

    def hat(position, cell):
        return jnp.maximum(1.0 - jnp.abs(position - cell), 0.0)

    def sample(values, offsets, head):
        info = coords[head]
        columns = [hat(info[8 + k : 9 + k], line_index) for k in range(POINTS)]
        blocks = []
        for offset in offsets:
            timed = info[12:16] * hat(info[0:4], first_frame + offset)
            for line in range(lines):
                share = timed * hat(info[4:8], first_line + line)
                total = share[0:1] * columns[0]
                for k in range(1, POINTS):
                    total = total + share[k : k + 1] * columns[k]
                blocks.append(total)
        corner = jnp.concatenate(blocks, axis=0).astype(BF)
        mine = values[pl.ds(pl.multiple_of(head * HD, HD), HD), :]
        return jnp.dot(mine, corner, preferred_element_type=F32)

    for c in range(width // 256):
        columns = slice(c * 256, (c + 1) * 256)
        vw_turned[columns, :] = vw[:, columns].T
    project_values(own_features, own_values)


    @pl.loop(0, AH, unroll=2)
    def _(head):
        sums[pl.ds(pl.multiple_of(head * HD, HD), HD), :] = sample(own_values, range(frames), head)

    loads[4].wait()
    span_cos, span_sin = span_turn[0, pl.ds(t, 1), :], span_turn[1, pl.ds(t, 1), :]
    cosine[...] = span_cos * row_turn[0] - span_sin * row_turn[1]
    sine[...] = span_sin * row_turn[0] + span_cos * row_turn[1]

    for i in range(q_heads):
        peak[i] = jnp.full((1, rows), masked, F32)
        denom[i] = jnp.zeros((1, rows), F32)
        numer[i] = jnp.zeros((HD, rows), F32)

    for i in range(2):

        @pl.when(t > 0)
        def _(i=i):
            up[i].wait_recv()

        @pl.when(t < spans - 1)
        def _(i=i):
            down[i].wait_recv()

        both = pl.ds(2 * i * per_frame, 2 * per_frame)
        if i == 1:
            loads[3].wait()
            wo_arrivals = wo_gather.arrivals()
            for _ in range(2 * chips - 2):
                next(wo_arrivals)
        project_values(halo.at[both], halo_values)

        @pl.loop(0, AH, unroll=2)
        def _(head, i=i):
            mine = pl.ds(pl.multiple_of(head * HD, HD), HD)
            total = sums[mine, :] + sample(halo_values, (-1 - i, frames + i), head)
            if i == 0:
                sums[mine, :] = total
            else:
                partial[:, mine] = total.T


    def part_rows(k, which):
        start, size = plan[k]
        return pl.ds(pl.multiple_of(start + which * (size // 2), 16), size // 2)

    def half_rows(k):
        start, size = plan[k]
        return pl.ds(start // 2, size // 2)

    def chunk_slice(k):
        start, size = plan[k]
        return slice(start, start + size)

    def chunk_span(k):
        return pl.ds(*plan[k])

    rs = []
    for k in range(chunks):
        rs_send[half_rows(k), :] = partial[part_rows(k, 1 - core), :].astype(BF)
        rs.append(
            remote(
                rs_send.at[half_rows(k)], rs_recv.at[half_rows(k)], rs_ss.at[k], rs_rs.at[k], {"mp": partner}
            )
        )
        rs[k].start()
    exchange = []

    def send_sums(k):
        rs[k].wait_recv()
        ex[chip, half_rows(k), :] = (
            partial[part_rows(k, core), :] + rs_recv[half_rows(k), :].astype(F32)
        ).astype(BF)
        if k > 0:
            for copy in exchange[k - 1]:
                copy.wait_send()
        copies = []
        for d in range(1, chips):
            mine = ex.at[chip, half_rows(k)]
            copies.append(
                remote(mine, mine, ex_ss.at[k, d - 1], ex_rs.at[k, d - 1], {"mp": (chip + d) % chips * 2 + core})
            )
            copies[-1].start()
        exchange.append(copies)

    send_sums(0)
    if chunks > 1:
        send_sums(1)
    loads[5].wait()
    for _ in wo_arrivals:
        pass

    vx_gathers, ab_copies, sq = [], [], []

    def mix(k):
        for copy in exchange[k]:
            copy.wait_recv()
        total = ex[0, half_rows(k), :].astype(F32)
        for c in range(1, chips):
            total = total + ex[c, half_rows(k), :].astype(F32)
        mixed = jnp.dot(total.astype(BF), wo[...].reshape(width, width), preferred_element_type=F32)
        ab[part_rows(k, core), :] = (queries[part_rows(k, core), :].astype(F32) + mixed).astype(BF)
        mine = ab.at[part_rows(k, core)]
        ab_copies.append(remote(mine, mine, ab_ss.at[k], ab_rs.at[k], {"mp": partner}))
        ab_copies[k].start()

    def project(k):
        ab_copies[k].wait_recv()
        size = plan[k][1]
        visual = jnp.dot(ab[chunk_slice(k), :], wp[...], preferred_element_type=F32)
        vx[me, chunk_slice(k), :] = (visual * flat(gain)).astype(BF)
        gather = Gather(
            lambda s, k=k: vx.at[s, chunk_span(k)],
            vx.at[me, chunk_span(k)],
            gather_sems(1 + k),
            groups,
            me,
        )
        squares = jnp.broadcast_to(jnp.sum(visual * visual, axis=1, keepdims=True), (size, HD))
        extra = -size % HD
        if extra:
            squares = jnp.concatenate([squares, jnp.zeros((extra, HD), F32)], axis=0)
        ssq[k, 0, :, 0 : size + extra] = squares.T[0:8]
        for d in range(1, groups):
            remote(ssq.at[k, 0], ssq.at[k, d], sq_ss.at[k], sq_rs.at[k], {"mp": (me + d) % groups}).start()
        rest = ssq.at[k, pl.ds(1, groups - 1)]
        sq.append(remote(rest, rest, sq_ss.at[k], sq_rs.at[k], {"mp": partner}))
        gather.near[0].start()
        vx_gathers.append(gather)

    def send_cross(k):
        if k > 0:
            for copy in vx_gathers[k - 1].cross[1:]:
                copy.wait_send()
        for copy in vx_gathers[k].cross[1:]:
            copy.start()

    tile = 256 if q_width % 256 == 0 else 128

    def slot_rows(slot):
        return pl.ds(pl.multiple_of(slot * model, 64), model)

    def add_cache(slot, span, first):
        term = jnp.dot(vx[slot, span, :], wc[slot_rows(slot), :], preferred_element_type=F32)
        kv_acc[span, :] = term if first else kv_acc[span, :] + term

    def add_query(slot, span, first):
        for c in range(q_width // tile):
            cols = slice(c * tile, (c + 1) * tile)
            term = jnp.dot(vx[slot, span, :], wq[slot_rows(slot), cols], preferred_element_type=F32)
            q_acc[span, cols] = term if first else q_acc[span, cols] + term

    def turn(x, cos, sin):
        return x * cos + pltpu.roll(x, HD // 2, 1) * sin

    def finish_cache(k):
        span = chunk_slice(k)
        square_sum = ssq[k, 0]
        sq[k].wait_recv()
        for d in range(1, groups):
            square_sum = square_sum + ssq[k, d]
        scale_row = lax.rsqrt(square_sum * (1.0 / (model * groups)) + epsilon)
        scale[span, :] = jnp.broadcast_to(scale_row[0:1], (HD, padded)).T[0 : plan[k][1]]
        bias = flat(cache_bias)
        for i in range(ch):
            is_key = me * ch + i < KVH
            cols = slice(i * HD, (i + 1) * HD)
            state = kv_acc[span, cols] * scale[span, :] + bias[:, cols]
            cos = jnp.where(is_key, cosine[span, :], 1.0)
            sin = jnp.where(is_key, sine[span, :], 0.0)
            state = turn(state, cos, sin).astype(BF)
            kv[t, me, span, cols] = state
            key_value[span, cols] = state

    def finish_query(k):
        span = chunk_slice(k)
        bias = flat(query_bias)
        for i in range(q_heads):
            cols = slice(i * HD, (i + 1) * HD)
            state = q_acc[span, cols] * scale[span, :] + bias[:, cols]
            state = turn(state, cosine[span, :], sine[span, :]) * (HD ** -0.5 * 1.4426950408889634)
            qs[i, span, :] = state.astype(BF)

    table = shared_heads(groups, q_heads, ch)

    early = pl.ds(0, plan[-1][0])

    def share_copy(d, which, span, entry):
        source, target, first, count, sent, received = entry
        block = kv.at[lax.rem(t + spans - d, spans), source, span, pl.ds(first * HD, count * HD)]
        return remote(block, block, d_ss.at[d, sent], d_rs.at[d, which, received], {"mp": target})

    def share(d, k):
        for entry in table:

            @pl.when(me == entry[0])
            def _(entry=entry):
                share_copy(d, k // (chunks - 1), chunk_span(k), entry).start()

    def share_wait(d, which):
        for entry in table:

            @pl.when(me == entry[1])
            def _(entry=entry):
                share_copy(d, which, chunk_span(chunks - 1) if which else early, entry).wait_recv()

    def share_drain(d):
        for entry in table:

            @pl.when(me == entry[0])
            def _(entry=entry):
                share_copy(d, 0, pl.ds(0, rows), entry).wait_send()

    def block_of(d, k):
        return kv.at[lax.rem(t + spans - d, spans), me, chunk_span(k)]

    def pass_copy(d, k):
        block = block_of(d, k)
        return remote(block, block, z_ss.at[d + 1], z_rs.at[d + 1, k], {"tm": (t + 1) % spans})

    def pass_on(d, k):
        @pl.when(t < spans - 1)
        def _():
            pass_copy(d, k).start()

    def hand_on(k):
        pass_on(0, k)
        share(0, k)

    def service(d, k):
        block = block_of(d, k)
        remote(block, block, z_ss.at[d], z_rs.at[d, k], {"tm": (t + spans - 1) % spans}).wait_recv()
        pass_on(d, k)
        share(d, k)

    def service_if(d, k):
        @pl.when(t >= d)
        def _():
            service(d, k)

    loads[6].wait()
    loads[7].wait()
    mix(0)
    send_sums(2)
    project(0)
    send_cross(0)
    mix(1)
    project(1)
    mix(2)
    project(2)
    everything = slice(0, rows)
    for k in range(chunks):
        span = chunk_slice(k)
        add_cache(me, span, True)
        if k == 0:
            gathered = [gather.arrivals() for gather in vx_gathers]
            near = next(gathered[0])
        arrivals = gathered[k]
        add_cache(near, span, False)
        if k == 0:
            send_cross(1)
        slots = []
        for d in range(1, chips):
            slots.append(next(arrivals))
            add_cache(slots[-1], span, False)
            if k > 0:
                add_query(slots[-1], span, False)
            for due in range(min(k, spans - 1) if d == 1 else 0):
                service_if(k - due, due)
            slots.append(next(arrivals))
            add_cache(slots[-1], span, False)
            if k > 0 and d < chips - 1:
                add_query(slots[-1], span, False)
        finish_cache(k)
        hand_on(k)
        if k == 0:
            for others in gathered[1:]:
                next(others)
            add_query(me, everything, True)
            add_query(near, everything, False)
            for slot in slots:
                add_query(slot, span, False)
        else:
            add_query(slots[-1], span, False)
        finish_query(k)
        if k == 0:
            send_cross(2)
    def attend(first, blocks, span, diagonal):
        length = blocks * (span.stop - span.start)

        beside = 3 if q_heads % 3 == 0 else 1

        @pl.loop(0, q_heads // beside)
        def _(n):
            heads = [n * beside + i for i in range(beside)]
            groups_of = [(me * q_heads + i) // GROUP for i in heads]
            old = [(peak[i], denom[i], numer[i]) for i in heads]

            def block(head):
                cols = pl.ds(pl.multiple_of(lax.rem(head, ch) * HD, HD), HD)
                return kv[pl.ds(first, blocks), head // ch, span, cols].reshape(length, HD)

            scores = [
                lax.dot_general(block(g), qs[i], (((1,), (1,)), ((), ())), preferred_element_type=F32)
                for i, g in zip(heads, groups_of)
            ]
            if diagonal:
                k_pos = lax.broadcasted_iota(jnp.int32, (length, rows), 0)
                q_pos = lax.broadcasted_iota(jnp.int32, (length, rows), 1)
                scores = [jnp.where(k_pos <= q_pos, x, masked) for x in scores]
            tops = [jnp.maximum(o[0], jnp.max(x, axis=0, keepdims=True)) for o, x in zip(old, scores)]
            weights = [jnp.exp2(x - top) for x, top in zip(scores, tops)]
            products = [
                lax.dot_general(
                    block(KVH + g), w.astype(BF), (((0,), (0,)), ((), ())), preferred_element_type=F32
                )
                for g, w in zip(groups_of, weights)
            ]
            added = [jnp.sum(w, axis=0, keepdims=True) for w in weights]
            for i, o, top, plus, product in zip(heads, old, tops, added, products):
                rescale = jnp.exp2(o[0] - top)
                peak[i] = top
                denom[i] = o[1] * rescale + plus
                numer[i] = o[2] * rescale + product

    most = min(3, spans - 1)

    def attend_earlier(span):
        @pl.loop(0, t // most)
        def _(n):
            attend(n * most, most, span, False)

        for left in range(1, most):

            @pl.when(lax.rem(t, most) == left)
            def _(left=left):
                attend(t - left, left, span, False)

    def wave(w):
        for k in range(chunks):
            d = w - k

            @pl.when((d >= 1) & (d <= t))
            def _(d=d, k=k):
                service(d, k)

    wave(chunks)
    share_wait(0, 0)
    share_wait(0, 1)
    attend(t, 1, everything, True)

    @pl.loop(chunks + 1, chunks + t)
    def _(w):
        wave(w)


    @pl.loop(1, t + 1)
    def _(d):
        share_wait(d, 0)

    attend_earlier(slice(0, plan[2][0]))

    @pl.loop(1, t + 1)
    def _(d):
        share_wait(d, 1)

    attend_earlier(slice(plan[2][0], rows))

    for i in range(q_heads):
        attention[:, i * HD : (i + 1) * HD] = (numer[i] / denom[i]).T.astype(BF)
    outs = [
        pltpu.make_async_copy(attention, attention_out, out_sem.at[0]),
        pltpu.make_async_copy(key_value, key_value_out, out_sem.at[1]),
    ]
    outs[0].start()
    outs[1].start()


    @pl.when(t < spans - 1)
    def _():
        for copy in up:
            copy.wait_send()

    @pl.when(t < spans - 1)
    def _():
        @pl.loop(0, t + 1)
        def _(d):
            block = kv.at[lax.rem(t + spans - d, spans), me]
            remote(block, block, z_ss.at[d + 1], z_rs.at[d + 1, 0], {"tm": (t + 1) % spans}).wait_send()

    @pl.when(t > 0)
    def _():
        for copy in down:
            copy.wait_send()

    @pl.loop(0, t + 1)
    def _(d):
        share_drain(d)

    wo_gather.drain()
    for k, gather in enumerate(vx_gathers):
        for copy in gather.near + ([] if k < chunks - 1 else gather.cross[1:]):
            copy.wait_send()
    for copy in rs + ab_copies + sq:
        copy.wait_send()
    for copy in exchange[-1]:
        copy.wait_send()
    for copy in outs:
        copy.wait()


def rows_first(x):
    return x.reshape(-1, HD) if x.shape[0] % HD == 0 else x[None]


def local(
    features,
    queries,
    anchor_frame,
    anchor_patch,
    time_offset,
    space_offset,
    value_weight,
    point_weight,
    point_bias,
    output_weight,
    project_weight,
    norm_gain,
    query_weight,
    query_bias,
    cache_weight,
    cache_bias,
):
    groups = lax.axis_size("mp")
    spans = lax.axis_size("tm")
    frames_here, patches_here, width = features.shape
    cells = frames_here * patches_here
    rows = queries.shape[0]
    plan = row_chunks(rows)
    chunks = len(plan)
    padded = max(-(-size // HD) * HD for _, size in plan)
    frequency = rope_base ** (-2.0 * np.arange(HD // 2, dtype=np.float64) / HD)
    sign = np.concatenate([-np.ones(HD // 2), np.ones(HD // 2)])

    def turns(positions):
        angles = positions[:, None] * np.concatenate([frequency, frequency])[None, :]
        return jnp.asarray(np.stack([np.cos(angles), np.sin(angles) * sign]).astype(np.float32))

    row_turn = turns(np.arange(rows, dtype=np.float64))
    span_turn = turns(np.arange(spans, dtype=np.float64) * rows)
    model = project_weight.shape[1]
    q_width = query_weight.shape[1]
    c_width = cache_weight.shape[1]
    q_heads = q_width // HD
    chips = groups // 2
    table = shared_heads(groups, q_heads, c_width // HD)
    most_sent = 1 + max(entry[4] for entry in table)
    most_received = 1 + max(entry[5] for entry in table)
    vmem = pl.BlockSpec(memory_space=pltpu.VMEM)
    hbm = pl.BlockSpec(memory_space=pltpu.HBM)
    dma = pltpu.SemaphoreType.DMA
    V = pltpu.VMEM
    return tuple(
        pl.pallas_call(
            functools.partial(kernel, groups, spans, frames_here, plan),
            out_shape=(
                jax.ShapeDtypeStruct((rows, q_width), BF),
                jax.ShapeDtypeStruct((rows, c_width), BF),
            ),
            in_specs=[hbm] * 3 + [vmem] * 10 + [hbm] * 5,
            out_specs=(pl.BlockSpec(memory_space=pl.ANY),) * 2,
            scratch_shapes=[
                V((rows, q_width), BF),
                V((rows, c_width), BF),
                V((cells, width), BF),
                V((rows, width), BF),
                V((2, rows, HD), F32),
                V((width, width), BF),
                V((groups, width // groups, width), BF),
                V((width, model), BF),
                V(query_weight.shape, BF),
                V(cache_weight.shape, BF),
                V((4 * patches_here, width), BF),
                V((width, cells), BF),
                V((width, 2 * patches_here), BF),
                V((rows, HD), F32),
                V((AH, 4 * POINTS, rows), F32),
                V((rows, HD), F32),
                V((rows, HD), F32),
                V((width, width), BF),
                V((width, rows), F32),
                V((rows, width), F32),
                V((rows // 2, width), BF),
                V((rows // 2, width), BF),
                V((chips, rows // 2, width), BF),
                V((rows, width), BF),
                V((groups, rows, model), BF),
                V((chunks, groups, 8, padded), F32),
                V((rows, HD), F32),
                V((rows, q_width), F32),
                V((rows, c_width), F32),
                V((q_heads, rows, HD), BF),
                V((spans, groups, rows, c_width), BF),
                V((q_heads, 1, rows), F32),
                V((q_heads, 1, rows), F32),
                V((q_heads, HD, rows), F32),
                dma((8,)),
                dma((2,)),
                dma((2, 2)),
                dma((2, 2)),
                dma((chunks,)),
                dma((chunks,)),
                dma((chunks, chips - 1)),
                dma((chunks, chips - 1)),
                dma((chunks,)),
                dma((chunks,)),
                dma((chunks,)),
                dma((chunks,)),
                dma((spans,)),
                dma((spans, chunks)),
                dma((spans, most_sent)),
                dma((spans, 2, most_received)),
                dma((1 + chunks, 4 * chips - 2)),
            ],
            compiler_params=pltpu.CompilerParams(
                collective_id=0, has_side_effects=True, vmem_limit_bytes=48 * 1024 * 1024
            ),
        )(
            *[
                pltpu.with_memory_space_constraint(x, pltpu.HBM)
                for x in (
                    features.reshape(cells, width),
                    queries,
                    row_turn,
                    anchor_frame[None],
                    anchor_patch[None],
                    time_offset.transpose(1, 2, 0),
                    space_offset.transpose(0, 2, 3, 1),
                    point_weight.T,
                    point_bias[None],
                    span_turn,
                    rows_first(norm_gain),
                    rows_first(query_bias),
                    rows_first(cache_bias),
                    value_weight,
                    output_weight,
                    project_weight,
                    query_weight,
                    cache_weight,
                )
            ]
        )
    )


def solution(mesh):
    return jax.shard_map(
        local,
        mesh=mesh,
        in_specs=(
            P(("dp", "tm"), "mp", None),
            P(("dp", "tm"), None),
            P(("dp", "tm")),
            P(("dp", "tm")),
            P(("dp", "tm"), None, None),
            P(None, ("dp", "tm"), None, None),
            P(),
            P(),
            P(),
            P("mp", None),
            P(None, "mp"),
            P("mp"),
            P(None, "mp"),
            P("mp"),
            P(None, "mp"),
            P("mp"),
        ),
        out_specs=(P(("dp", "tm"), "mp"), P(("dp", "tm"), "mp")),
        check_vma=False,
    )
```
